16 devices in a mesh: data: 2 (over y, z), seq: 8 (over x, core).
Axes of the slice: x: 4, y: 2, z: 1, core: 2. Of those that a mesh axis runs over, the one named last changes fastest.
The devices are a block of a 4x4x8 slice.
Arguments:
- act_in: bfloat16 [8, 2048, 1024], P('data', 'seq'), parts along dimension 0
- ln1_scale: float32 [1024], replicated
- ln1_bias: float32 [1024], replicated
- w_in: bfloat16 [1024, 4096], replicated
- b_in: float32 [4096], replicated
- ln2_scale: float32 [2048], replicated
- ln2_bias: float32 [2048], replicated
- w_spatial: bfloat16 [2048, 2048], replicated
- b_spatial: float32 [2048], replicated
- causal_mask: int32 [2048, 2048], replicated
- w_out: bfloat16 [2048, 1024], replicated
- b_out: float32 [1024], replicated
Outputs:
- output: bfloat16 [8, 2048, 1024], P('data', 'seq'), parts along dimension 0
There are 2 independent parts. The reference program is written for one: setup_inputs(seed, part) draws one part's arguments, and reference() takes and returns one part's arrays. A program takes and returns all parts, laid end to end along the dimension named above; an argument that names none is the same for every part.
All inputs are finite; a program needn't handle non-finite values.
Results may differ from the reference program's by a relative error of at most 0.0115268.
Values are sent between devices in bfloat16 or wider.
A program may use at most 768 MiB of HBM per device.

```python
import jax
import jax.numpy as jnp
from jax import lax

BATCH_ROWS = 4
SEQ_LEN = 2048
MODEL_DIM = 1024
FFN_DIM = 4096
GATE_DIM = FFN_DIM // 2
LN_EPS = 1e-6


def layer_norm(features, ln_gain, ln_shift):
    mean_val = jnp.mean(features, axis=-1, keepdims=True)
    centered = features - mean_val
    var_val = jnp.mean(centered * centered, axis=-1, keepdims=True)
    return centered * lax.rsqrt(var_val + LN_EPS) * ln_gain + ln_shift


def draw_mask(mask_key):
    cut_points = jax.random.randint(mask_key, (2,), 1, SEQ_LEN)
    positions = jnp.arange(SEQ_LEN)
    doc_id = jnp.sum(positions[:, None] >= cut_points[None, :], axis=1)
    keep_mask = (positions[None, :] <= positions[:, None]) & (doc_id[None, :] == doc_id[:, None])
    return keep_mask.astype(jnp.int32)


def setup_inputs(seed: int = 0, part: int = 0) -> dict:
    key_list = jax.random.split(jax.random.key(seed), 12)
    x_key = jax.random.fold_in(key_list[0], part)
    causal_mask = draw_mask(key_list[7])
    row_count = jnp.sum(causal_mask, axis=1).astype(jnp.float32)
    act_in = jax.random.normal(x_key, (BATCH_ROWS, SEQ_LEN, MODEL_DIM), jnp.float32)
    ln1_scale = 1.0 + 0.5 * jax.random.normal(key_list[1], (MODEL_DIM,), jnp.float32)
    ln1_bias = 0.5 * jax.random.normal(key_list[2], (MODEL_DIM,), jnp.float32)
    w_in = jax.random.normal(key_list[3], (MODEL_DIM, FFN_DIM), jnp.float32) * MODEL_DIM ** -0.5
    b_in = 0.5 * jax.random.normal(key_list[4], (FFN_DIM,), jnp.float32)
    ln2_scale = 1.0 + 0.5 * jax.random.normal(key_list[5], (GATE_DIM,), jnp.float32)
    ln2_bias = 0.5 * jax.random.normal(key_list[6], (GATE_DIM,), jnp.float32)
    w_spatial = jax.random.normal(key_list[8], (SEQ_LEN, SEQ_LEN), jnp.float32) * lax.rsqrt(row_count)[:, None]
    b_spatial = 1.0 + 0.8 * jax.random.normal(key_list[9], (SEQ_LEN,), jnp.float32)
    w_out = jax.random.normal(key_list[10], (GATE_DIM, MODEL_DIM), jnp.float32) * (2.0 * GATE_DIM ** -0.5)
    b_out = 0.3 * jax.random.normal(key_list[11], (MODEL_DIM,), jnp.float32)
    return dict(
        act_in=act_in.astype(jnp.bfloat16),
        ln1_scale=ln1_scale,
        ln1_bias=ln1_bias,
        w_in=w_in.astype(jnp.bfloat16),
        b_in=b_in,
        ln2_scale=ln2_scale,
        ln2_bias=ln2_bias,
        w_spatial=w_spatial.astype(jnp.bfloat16),
        b_spatial=b_spatial,
        causal_mask=causal_mask,
        w_out=w_out.astype(jnp.bfloat16),
        b_out=b_out,
    )


def reference(act_in, ln1_scale, ln1_bias, w_in, b_in, ln2_scale, ln2_bias, w_spatial, b_spatial, causal_mask, w_out, b_out):
    w_masked = jnp.where(causal_mask > 0, w_spatial, jnp.zeros_like(w_spatial))

    def one_sequence(seq_act):
        normed = layer_norm(seq_act.astype(jnp.float32), ln1_scale, ln1_bias).astype(jnp.bfloat16)
        hidden = jax.nn.gelu(jnp.dot(normed, w_in, preferred_element_type=jnp.float32) + b_in, approximate=True).astype(jnp.bfloat16)
        gate_half = hidden[:, :GATE_DIM]
        value_norm = layer_norm(hidden[:, GATE_DIM:].astype(jnp.float32), ln2_scale, ln2_bias).astype(jnp.bfloat16)
        spatial = (jnp.dot(w_masked, value_norm, preferred_element_type=jnp.float32) + b_spatial[:, None]).astype(jnp.bfloat16)
        gated_act = (gate_half.astype(jnp.float32) * spatial.astype(jnp.float32)).astype(jnp.bfloat16)
        projected = jnp.dot(gated_act, w_out, preferred_element_type=jnp.float32) + b_out
        return (seq_act.astype(jnp.float32) + projected).astype(jnp.bfloat16)

    return lax.map(one_sequence, act_in)
```

```python
import functools

import jax
import jax.numpy as jnp
from jax import lax
from jax.experimental import pallas as pl
from jax.experimental.pallas import tpu as pltpu
from jax.sharding import PartitionSpec as P

LN_EPS = 1e-6
MESH = pl.DeviceIdType.MESH
F32 = jnp.float32
BF16 = jnp.bfloat16

V, W, O, M = 0, 4, 8, 12
SCHEDULES = (
    (V + 0, M, V + 1, W + 0, W + 1, O + 1, V + 3, V + 2, W + 2, O + 2, W + 3, O + 3, O + 0),
    (V + 1, M, V + 0, W + 0, O + 0, V + 2, W + 1, W + 2, O + 2, V + 3, W + 3, O + 3, O + 1),
    (V + 2, M, V + 0, W + 0, O + 0, V + 1, W + 1, O + 1, V + 3, W + 2, W + 3, O + 3, O + 2),
    (V + 3, M, V + 0, W + 0, O + 0, V + 2, V + 1, W + 1, O + 1, W + 2, O + 2, W + 3, O + 3),
)
HALF = 7


def pack(steps):
    return sum(s << (4 * i) for i, s in enumerate(steps))


def layer_norm_rows(rows, gain, shift):
    mean = jnp.mean(rows, axis=-1, keepdims=True)
    centered = rows - mean
    var = jnp.mean(centered * centered, axis=-1, keepdims=True)
    return centered * lax.rsqrt(var + LN_EPS) * gain + shift


def gelu(a):
    c0 = 0.7978845608028654
    inner = a * (c0 + (c0 * 0.044715) * (a * a))
    return a * (0.5 + 0.5 * jnp.tanh(inner))


def kernel(cores, x_ref, ln1s_h, ln1b_h, win_h, bin_h, ln2s_h, ln2b_h, wsp_h, bsp_h, mask_h, wout_h, bout_h, out_ref,
           xbuf, u, h, vn, wm, mask, win, wout, q, obuf, ln1s, ln1b, b_in, ln2s, ln2b, bsp, bout,
           small_sem, win_sem, wout_sem, wsp_sem, mask_sem, xs_sem, xr_sem, vs_sem, vr_sem, os_sem, or_sem):
    data, me = lax.axis_index("data"), lax.axis_index("seq")
    chip, core = me // cores, me % cores
    partner = (data, chip * cores + (cores - 1 - core))
    chips, rows, width = x_ref.shape
    gate = wout_h.shape[0]

    def block_of(k):
        return k * cores + core

    def row_slice(k):
        return pl.ds(pl.multiple_of(block_of(k) * rows, rows), rows)

    own = pltpu.make_async_copy(x_ref.at[chip], xbuf.at[chip], xr_sem.at[chip])
    own.start()
    smalls = [pltpu.make_async_copy(src, dst, small_sem.at[i]) for i, (src, dst) in enumerate(
        ((ln1s_h, ln1s), (ln1b_h, ln1b), (bin_h, b_in), (ln2s_h, ln2s), (ln2b_h, ln2b), (bsp_h, bsp), (bout_h, bout)))]
    for cp in smalls:
        cp.start()
    win_v = pltpu.make_async_copy(win_h.at[:, pl.ds(gate, gate)], win.at[:, pl.ds(gate, gate)], win_sem.at[0])
    win_g = pltpu.make_async_copy(win_h.at[:, pl.ds(0, gate)], win.at[:, pl.ds(0, gate)], win_sem.at[1])
    win_v.start()

    barrier = pltpu.get_barrier_semaphore()
    pl.semaphore_signal(barrier, inc=1, device_id=partner, device_id_type=MESH)
    for d in range(1, chips):
        pl.semaphore_signal(barrier, inc=1, device_id=(data, (chip + d) % chips * cores + core), device_id_type=MESH)
    pl.semaphore_wait(barrier, chips)

    def send_x(d):
        to = (chip + d) % chips
        pltpu.make_async_remote_copy(
            src_ref=x_ref.at[to], dst_ref=xbuf.at[chip], send_sem=xs_sem.at[d - 1], recv_sem=xr_sem.at[chip],
            device_id=(data, to * cores + core), device_id_type=MESH).start()

    @pl.when(chip == 0)
    def _():
        send_x(chips // 2)

    for d in range(1, chips):
        if d != chips // 2:
            send_x(d)

    @pl.when(chip != 0)
    def _():
        send_x(chips // 2)

    win_g.start()
    spatial_loads = []
    for k in range(chips):
        cols = pl.ds(0, (k + 1) * cores * rows)
        a = pltpu.make_async_copy(wsp_h.at[row_slice(k), cols], wm.at[k, :, cols], wsp_sem.at[k])
        b = pltpu.make_async_copy(mask_h.at[row_slice(k), cols], mask.at[k, :, cols], mask_sem.at[k])
        a.start()
        b.start()
        spatial_loads += [a, b]
    wout_load = pltpu.make_async_copy(wout_h, wout, wout_sem)
    wout_load.start()

    def dense_tiles(k, first, count, tile):
        def body(t, carry):
            cols = pl.ds(pl.multiple_of(first + t * tile, tile), tile)
            a = jnp.dot(u[...], win[:, cols], preferred_element_type=F32) + b_in[:, cols]
            h[k, :, cols] = gelu(a).astype(BF16)
            return carry
        lax.fori_loop(0, count, body, 0)

    def vn_copy(k):
        return pltpu.make_async_remote_copy(
            src_ref=vn.at[row_slice(k), :], dst_ref=vn.at[row_slice(k), :], send_sem=vs_sem.at[k], recv_sem=vr_sem.at[k],
            device_id=partner, device_id_type=MESH)

    def do_v(k):
        pltpu.make_async_copy(xbuf.at[k], xbuf.at[k], xr_sem.at[k]).wait()

        @pl.when(k == chip)
        def _():
            for cp in smalls:
                cp.wait()

        chunk = 32

        def ln1_body(r, carry):
            rs = pl.ds(pl.multiple_of(r * chunk, chunk), chunk)
            u[rs, :] = layer_norm_rows(xbuf[k, rs, :].astype(F32), ln1s[...], ln1b[...]).astype(BF16)
            return carry
        lax.fori_loop(0, rows // chunk, ln1_body, 0, unroll=2)

        @pl.when(k == chip)
        def _():
            win_v.wait()
        tile = gate // 4
        dense_tiles(k, gate, 4, tile)
        chunk2 = 16
        base = block_of(k) * rows

        def ln2_body(r, carry):
            rs = pl.ds(pl.multiple_of(r * chunk2, chunk2), chunk2)
            ws = pl.ds(pl.multiple_of(base + r * chunk2, chunk2), chunk2)
            vn[ws, :] = layer_norm_rows(h[k, rs, gate:].astype(F32), ln2s[...], ln2b[...]).astype(BF16)
            return carry
        lax.fori_loop(0, rows // chunk2, ln2_body, 0, unroll=2)
        vn_copy(k).start()

        @pl.when(k == chip)
        def _():
            win_g.wait()
        dense_tiles(k, 0, 4, tile)

    def do_mask():
        for cp in spatial_loads:
            cp.wait()
        chunk = 32
        for k in range(chips):
            cols = slice(0, (k + 1) * cores * rows)

            def body(r, carry):
                rs = pl.ds(pl.multiple_of(r * chunk, chunk), chunk)
                keep = mask[k, rs, cols] > 0
                wm[k, rs, cols] = jnp.where(keep, wm[k, rs, cols].astype(F32), 0.0).astype(BF16)
                return carry
            lax.fori_loop(0, rows // chunk, body, 0)
        wout_load.wait()

    def do_o(k):
        bias_row = bsp[:, row_slice(k)]
        bias = jnp.transpose(jnp.broadcast_to(bias_row, (128, rows)))[:, :1]
        for kk in range(chips):
            @pl.when(k == kk)
            def _():
                depth = (kk + 1) * cores * rows
                tile = gate // 4

                def body(t, carry):
                    cols = pl.ds(pl.multiple_of(t * tile, tile), tile)
                    s = jnp.dot(wm[kk, :, :depth], vn[:depth, cols], preferred_element_type=F32) + bias
                    q[:, cols] = (h[kk, :, cols].astype(F32) * s.astype(BF16).astype(F32)).astype(BF16)
                    return carry
                lax.fori_loop(0, gate // tile, body, 0)
        tile = width // 2

        def out_body(t, carry):
            cols = pl.ds(pl.multiple_of(t * tile, tile), tile)
            y = jnp.dot(q[...], wout[:, cols], preferred_element_type=F32) + bout[:, cols]
            obuf[k, :, cols] = (xbuf[k, :, cols].astype(F32) + y).astype(BF16)
            return carry
        lax.fori_loop(0, width // tile, out_body, 0)

        @pl.when(k == chip)
        def _():
            pltpu.make_async_copy(obuf.at[k], out_ref.at[chip], or_sem.at[chip]).start()

        @pl.when(k != chip)
        def _():
            out_copy(k).start()

    def out_copy(k):
        return pltpu.make_async_remote_copy(
            src_ref=obuf.at[k], dst_ref=out_ref.at[chip], send_sem=os_sem.at[k], recv_sem=or_sem.at[chip],
            device_id=(data, k * cores + core), device_id_type=MESH)

    low = high = jnp.int32(0)
    for c, steps in enumerate(SCHEDULES):
        low = jnp.where(chip == c, pack(steps[:HALF]), low)
        high = jnp.where(chip == c, pack(steps[HALF:]), high)

    def step(i, carry):
        code = jnp.where(i < HALF, low, high)
        action = lax.shift_right_logical(code, 4 * (i % HALF)) % 16
        k = action % 4

        @pl.when(action // 4 == V // 4)
        def _():
            do_v(k)

        @pl.when(action // 4 == W // 4)
        def _():
            vn_copy(k).wait_recv()

        @pl.when(action // 4 == O // 4)
        def _():
            do_o(k)

        @pl.when(action // 4 == M // 4)
        def _():
            do_mask()
        return carry
    lax.fori_loop(0, len(SCHEDULES[0]), step, 0)

    for d in range(1, chips):
        to = (chip + d) % chips
        pltpu.make_async_remote_copy(
            src_ref=x_ref.at[to], dst_ref=xbuf.at[chip], send_sem=xs_sem.at[d - 1], recv_sem=xr_sem.at[chip],
            device_id=(data, to * cores + core), device_id_type=MESH).wait_send()
    for k in range(chips):
        vn_copy(k).wait_send()

        @pl.when(k != chip)
        def _():
            out_copy(k).wait_send()
    for k in range(chips):
        pltpu.make_async_copy(out_ref.at[k], out_ref.at[k], or_sem.at[k]).wait()


def solution(mesh):
    row_spec = P('data', 'seq', None)
    replicated = P()

    def local_block(act_in, ln1_scale, ln1_bias, w_in, b_in, ln2_scale, ln2_bias, w_spatial, b_spatial, causal_mask, w_out, b_out):
        chips, rows, width = act_in.shape
        cores = mesh.shape['seq'] // chips
        ffn, gate, total = w_in.shape[1], w_out.shape[0], w_spatial.shape[0]
        any_spec = pl.BlockSpec(memory_space=pl.ANY)
        row = lambda a: a.reshape(1, -1)
        dma = pltpu.SemaphoreType.DMA
        return pl.pallas_call(
            functools.partial(kernel, cores),
            out_shape=jax.ShapeDtypeStruct(act_in.shape, act_in.dtype),
            in_specs=[any_spec] * 12,
            out_specs=any_spec,
            scratch_shapes=[
                pltpu.VMEM((chips, rows, width), BF16),
                pltpu.VMEM((rows, width), BF16),
                pltpu.VMEM((chips, rows, ffn), BF16),
                pltpu.VMEM((total, gate), BF16),
                pltpu.VMEM((chips, rows, total), BF16),
                pltpu.VMEM((chips, rows, total), jnp.int32),
                pltpu.VMEM((width, ffn), BF16),
                pltpu.VMEM((gate, width), BF16),
                pltpu.VMEM((rows, gate), BF16),
                pltpu.VMEM((chips, rows, width), BF16),
                pltpu.VMEM((1, width), F32),
                pltpu.VMEM((1, width), F32),
                pltpu.VMEM((1, ffn), F32),
                pltpu.VMEM((1, gate), F32),
                pltpu.VMEM((1, gate), F32),
                pltpu.VMEM((1, total), F32),
                pltpu.VMEM((1, width), F32),
                dma((7,)), dma((2,)), dma, dma((chips,)), dma((chips,)),
                dma((chips - 1,)), dma((chips,)), dma((chips,)), dma((chips,)), dma((chips,)), dma((chips,)),
            ],
            compiler_params=pltpu.CompilerParams(collective_id=0, has_side_effects=True, vmem_limit_bytes=66_000_000),
        )(act_in, row(ln1_scale), row(ln1_bias), w_in, row(b_in), row(ln2_scale), row(ln2_bias), w_spatial, row(b_spatial),
          causal_mask, w_out, row(b_out))

    return jax.shard_map(local_block, mesh=mesh, in_specs=(row_spec,) + (replicated,) * 11, out_specs=row_spec, check_vma=False)
```

```python
import functools

import jax
import jax.numpy as jnp
from jax import lax
from jax.experimental import pallas as pl
from jax.experimental.pallas import tpu as pltpu
from jax.sharding import PartitionSpec as P

LN_EPS = 1e-6
MESH = pl.DeviceIdType.MESH
F32 = jnp.float32
BF16 = jnp.bfloat16

V, W, O, M = 0, 4, 8, 12
SCHEDULES = (
    (V + 0, M, V + 1, V + 3, W + 0, W + 1, O + 1, V + 2, W + 2, O + 2, W + 3, O + 3, O + 0),
    (V + 1, M, V + 0, V + 2, W + 0, O + 0, V + 3, W + 1, W + 2, O + 2, W + 3, O + 3, O + 1),
    (V + 2, M, V + 1, V + 3, V + 0, W + 0, O + 0, W + 1, O + 1, W + 2, W + 3, O + 3, O + 2),
    (V + 3, M, V + 0, V + 2, W + 0, O + 0, V + 1, W + 1, O + 1, W + 2, O + 2, W + 3, O + 3),
)
HALF = 7


def pack(steps):
    return sum(s << (4 * i) for i, s in enumerate(steps))


def layer_norm_rows(rows, gain, shift):
    mean = jnp.mean(rows, axis=-1, keepdims=True)
    centered = rows - mean
    var = jnp.mean(centered * centered, axis=-1, keepdims=True)
    return centered * lax.rsqrt(var + LN_EPS) * gain + shift


def gelu(a):
    c0 = 0.7978845608028654
    inner = a * (c0 + (c0 * 0.044715) * (a * a))
    return a * (0.5 + 0.5 * jnp.tanh(inner))


def kernel(cores, x_ref, ln1s_h, ln1b_h, win_h, bin_h, ln2s_h, ln2b_h, wsp_h, bsp_h, mask_h, wout_h, bout_h, out_ref,
           xbuf, u, hv, g, vn, wm, mask, win, wout, q, obuf, ln1s, ln1b, b_in, ln2s, ln2b, bsp, bout,
           small_sem, win_sem, wout_sem, wsp_sem, mask_sem, xs_sem, xr_sem, vs_sem, vr_sem, os_sem, or_sem):
    data, me = lax.axis_index("data"), lax.axis_index("seq")
    chip, core = me // cores, me % cores
    partner = (data, chip * cores + (cores - 1 - core))
    chips, rows, width = x_ref.shape
    gate = wout_h.shape[0]

    def block_of(k):
        return k * cores + core

    def row_slice(k):
        return pl.ds(pl.multiple_of(block_of(k) * rows, rows), rows)

    own = pltpu.make_async_copy(x_ref.at[chip], xbuf.at[chip], xr_sem.at[chip])
    own.start()
    smalls = [pltpu.make_async_copy(src, dst, small_sem.at[i]) for i, (src, dst) in enumerate(
        ((ln1s_h, ln1s), (ln1b_h, ln1b), (bin_h, b_in), (ln2s_h, ln2s), (ln2b_h, ln2b), (bsp_h, bsp), (bout_h, bout)))]
    for cp in smalls:
        cp.start()
    win_v = pltpu.make_async_copy(win_h.at[:, pl.ds(gate, gate)], win.at[:, pl.ds(gate, gate)], win_sem.at[0])
    win_g = pltpu.make_async_copy(win_h.at[:, pl.ds(0, gate)], win.at[:, pl.ds(0, gate)], win_sem.at[1])
    win_v.start()

    barrier = pltpu.get_barrier_semaphore()
    pl.semaphore_signal(barrier, inc=1, device_id=partner, device_id_type=MESH)
    for d in range(1, chips):
        pl.semaphore_signal(barrier, inc=1, device_id=(data, (chip + d) % chips * cores + core), device_id_type=MESH)
    pl.semaphore_wait(barrier, chips)

    def send_x(d):
        to = (chip + d) % chips
        pltpu.make_async_remote_copy(
            src_ref=x_ref.at[to], dst_ref=xbuf.at[chip], send_sem=xs_sem.at[d - 1], recv_sem=xr_sem.at[chip],
            device_id=(data, to * cores + core), device_id_type=MESH).start()

    for d in (*(d for d in range(1, chips) if d != chips // 2), chips // 2):
        send_x(d)

    win_g.start()
    spatial_loads = []
    for k in range(chips):
        cols = pl.ds(0, (k + 1) * cores * rows)
        a = pltpu.make_async_copy(wsp_h.at[row_slice(k), cols], wm.at[k, :, cols], wsp_sem.at[k])
        b = pltpu.make_async_copy(mask_h.at[row_slice(k), cols], mask.at[k, :, cols], mask_sem.at[k])
        a.start()
        b.start()
        spatial_loads += [a, b]
    wout_load = pltpu.make_async_copy(wout_h, wout, wout_sem)
    wout_load.start()

    tile = gate // 4

    def dense(cols):
        a = jnp.dot(u[...], win[:, cols], preferred_element_type=F32) + b_in[:, cols]
        return gelu(a).astype(BF16)

    def vn_copy(k):
        return pltpu.make_async_remote_copy(
            src_ref=vn.at[row_slice(k), :], dst_ref=vn.at[row_slice(k), :], send_sem=vs_sem.at[k], recv_sem=vr_sem.at[k],
            device_id=partner, device_id_type=MESH)

    def do_v(k):
        pltpu.make_async_copy(xbuf.at[k], xbuf.at[k], xr_sem.at[k]).wait()

        @pl.when(k == chip)
        def _():
            for cp in smalls:
                cp.wait()

        chunk = 32

        def ln1_body(r, carry):
            rs = pl.ds(pl.multiple_of(r * chunk, chunk), chunk)
            u[rs, :] = layer_norm_rows(xbuf[k, rs, :].astype(F32), ln1s[...], ln1b[...]).astype(BF16)
            return carry
        lax.fori_loop(0, rows // chunk, ln1_body, 0, unroll=4)

        @pl.when(k == chip)
        def _():
            win_v.wait()

        def value_body(t, carry):
            start = pl.multiple_of(t * tile, tile)
            hv[:, pl.ds(start, tile)] = dense(pl.ds(gate + start, tile))
            return carry
        lax.fori_loop(0, gate // tile, value_body, 0, unroll=True)

        @pl.when(k == chip)
        def _():
            win_g.wait()
        chunk2 = 16
        base = block_of(k) * rows
        per_tile = rows // chunk2 // (gate // tile)

        def gate_body(t, carry):
            cols = pl.ds(pl.multiple_of(t * tile, tile), tile)
            g[k, :, cols] = dense(cols)
            for r in range(per_tile):
                first = (t * per_tile + r) * chunk2
                rs = pl.ds(pl.multiple_of(first, chunk2), chunk2)
                ws = pl.ds(pl.multiple_of(base + first, chunk2), chunk2)
                vn[ws, :] = layer_norm_rows(hv[rs, :].astype(F32), ln2s[...], ln2b[...]).astype(BF16)
            return carry
        lax.fori_loop(0, gate // tile, gate_body, 0, unroll=True)
        vn_copy(k).start()

    def do_mask():
        for cp in spatial_loads:
            cp.wait()
        chunk = 32
        for k in range(chips):
            cols = slice(0, (k + 1) * cores * rows)

            def body(r, carry):
                rs = pl.ds(pl.multiple_of(r * chunk, chunk), chunk)
                keep = mask[k, rs, cols] > 0
                wm[k, rs, cols] = jnp.where(keep, wm[k, rs, cols].astype(F32), 0.0).astype(BF16)
                return carry
            lax.fori_loop(0, rows // chunk, body, 0)
        wout_load.wait()

    def do_o(k):
        bias_row = bsp[:, row_slice(k)]
        bias = jnp.transpose(jnp.broadcast_to(bias_row, (128, rows)))[:, :1]
        for kk in range(chips):
            @pl.when(k == kk)
            def _():
                depth = (kk + 1) * cores * rows
                def body(t, carry):
                    cols = pl.ds(pl.multiple_of(t * tile, tile), tile)
                    s = jnp.dot(wm[kk, :, :depth], vn[:depth, cols], preferred_element_type=F32) + bias
                    q[:, cols] = (g[kk, :, cols].astype(F32) * s.astype(BF16).astype(F32)).astype(BF16)
                    return carry
                lax.fori_loop(0, gate // tile, body, 0, unroll=True)
        out_tile = width // 2

        def out_body(t, carry):
            cols = pl.ds(pl.multiple_of(t * out_tile, out_tile), out_tile)
            y = jnp.dot(q[...], wout[:, cols], preferred_element_type=F32) + bout[:, cols]
            obuf[k, :, cols] = (xbuf[k, :, cols].astype(F32) + y).astype(BF16)
            return carry
        lax.fori_loop(0, width // out_tile, out_body, 0, unroll=True)

        @pl.when(k == chip)
        def _():
            pltpu.make_async_copy(obuf.at[k], out_ref.at[chip], or_sem.at[chip]).start()

        @pl.when(k != chip)
        def _():
            out_copy(k).start()

    def out_copy(k):
        return pltpu.make_async_remote_copy(
            src_ref=obuf.at[k], dst_ref=out_ref.at[chip], send_sem=os_sem.at[k], recv_sem=or_sem.at[chip],
            device_id=(data, k * cores + core), device_id_type=MESH)

    low = high = jnp.int32(0)
    for c, steps in enumerate(SCHEDULES):
        low = jnp.where(chip == c, pack(steps[:HALF]), low)
        high = jnp.where(chip == c, pack(steps[HALF:]), high)

    def step(i, carry):
        code = jnp.where(i < HALF, low, high)
        action = lax.shift_right_logical(code, 4 * (i % HALF)) % 16
        k = action % 4

        @pl.when(action // 4 == V // 4)
        def _():
            do_v(k)

        @pl.when(action // 4 == W // 4)
        def _():
            vn_copy(k).wait_recv()

        @pl.when(action // 4 == O // 4)
        def _():
            do_o(k)

        @pl.when(action // 4 == M // 4)
        def _():
            do_mask()
        return carry
    lax.fori_loop(0, len(SCHEDULES[0]), step, 0)

    for d in range(1, chips):
        to = (chip + d) % chips
        pltpu.make_async_remote_copy(
            src_ref=x_ref.at[to], dst_ref=xbuf.at[chip], send_sem=xs_sem.at[d - 1], recv_sem=xr_sem.at[chip],
            device_id=(data, to * cores + core), device_id_type=MESH).wait_send()
    for k in range(chips):
        vn_copy(k).wait_send()

        @pl.when(k != chip)
        def _():
            out_copy(k).wait_send()
    for k in range(chips):
        pltpu.make_async_copy(out_ref.at[k], out_ref.at[k], or_sem.at[k]).wait()


def solution(mesh):
    row_spec = P('data', 'seq', None)
    replicated = P()

    def local_block(act_in, ln1_scale, ln1_bias, w_in, b_in, ln2_scale, ln2_bias, w_spatial, b_spatial, causal_mask, w_out, b_out):
        chips, rows, width = act_in.shape
        cores = mesh.shape['seq'] // chips
        ffn, gate, total = w_in.shape[1], w_out.shape[0], w_spatial.shape[0]
        any_spec = pl.BlockSpec(memory_space=pl.ANY)
        row = lambda a: a.reshape(1, -1)
        dma = pltpu.SemaphoreType.DMA
        return pl.pallas_call(
            functools.partial(kernel, cores),
            out_shape=jax.ShapeDtypeStruct(act_in.shape, act_in.dtype),
            in_specs=[any_spec] * 12,
            out_specs=any_spec,
            scratch_shapes=[
                pltpu.VMEM((chips, rows, width), BF16),
                pltpu.VMEM((rows, width), BF16),
                pltpu.VMEM((rows, gate), BF16),
                pltpu.VMEM((chips, rows, gate), BF16),
                pltpu.VMEM((total, gate), BF16),
                pltpu.VMEM((chips, rows, total), BF16),
                pltpu.VMEM((chips, rows, total), jnp.int32),
                pltpu.VMEM((width, ffn), BF16),
                pltpu.VMEM((gate, width), BF16),
                pltpu.VMEM((rows, gate), BF16),
                pltpu.VMEM((chips, rows, width), BF16),
                pltpu.VMEM((1, width), F32),
                pltpu.VMEM((1, width), F32),
                pltpu.VMEM((1, ffn), F32),
                pltpu.VMEM((1, gate), F32),
                pltpu.VMEM((1, gate), F32),
                pltpu.VMEM((1, total), F32),
                pltpu.VMEM((1, width), F32),
                dma((7,)), dma((2,)), dma, dma((chips,)), dma((chips,)),
                dma((chips - 1,)), dma((chips,)), dma((chips,)), dma((chips,)), dma((chips,)), dma((chips,)),
            ],
            compiler_params=pltpu.CompilerParams(collective_id=0, has_side_effects=True, vmem_limit_bytes=66_000_000),
        )(act_in, row(ln1_scale), row(ln1_bias), w_in, row(b_in), row(ln2_scale), row(ln2_bias), w_spatial, row(b_spatial),
          causal_mask, w_out, row(b_out))

    return jax.shard_map(local_block, mesh=mesh, in_specs=(row_spec,) + (replicated,) * 11, out_specs=row_spec, check_vma=False)
```

```python
import functools

import jax
import jax.numpy as jnp
from jax import lax
from jax.experimental import pallas as pl
from jax.experimental.pallas import tpu as pltpu
from jax.sharding import PartitionSpec as P

LN_EPS = 1e-6
MESH = pl.DeviceIdType.MESH
F32 = jnp.float32
BF16 = jnp.bfloat16

HALVES = 2


def V(k, half):
    return k * HALVES + half


def O(k, half):
    return 12 + k * HALVES + half


W, O_FIRST, G, BITS, PER_WORD = 8, 12, 20, 5, 6
SCHEDULES = (
    (V(1, 0), V(3, 0), V(1, 1), V(3, 1), V(2, 0), W + 0, W + 1, O(1, 0), O(1, 1), V(2, 1), W + 2, W + 3,
     O(3, 0), O(3, 1), G, O(2, 0), O(2, 1), O(0, 0), O(0, 1)),
    (V(0, 0), V(2, 0), V(0, 1), V(2, 1), W + 0, W + 1, O(0, 0), O(0, 1), V(3, 0), W + 2, O(2, 0), O(2, 1), V(3, 1), W + 3,
     O(3, 0), G, O(3, 1), O(1, 0), O(1, 1)),
    (V(1, 0), V(3, 0), V(1, 1), V(3, 1), V(0, 0), V(0, 1), W + 0, W + 1, O(1, 0), O(0, 0), O(1, 1), G, O(0, 1), W + 2, W + 3,
     O(3, 0), O(3, 1), O(2, 0), O(2, 1)),
    (V(0, 0), V(2, 0), V(0, 1), V(2, 1), W + 0, O(0, 0), O(0, 1), V(1, 0), V(1, 1), W + 1, O(1, 0), W + 2, O(2, 0), G,
     O(1, 1), O(2, 1), W + 3, O(3, 0), O(3, 1)),
)


def pack(steps):
    return sum(s << (BITS * i) for i, s in enumerate(steps))


def layer_norm_rows(rows, gain, shift):
    mean = jnp.mean(rows, axis=-1, keepdims=True)
    centered = rows - mean
    var = jnp.mean(centered * centered, axis=-1, keepdims=True)
    return centered * lax.rsqrt(var + LN_EPS) * gain + shift


def gelu(a):
    c0 = 0.7978845608028654
    inner = a * (c0 + (c0 * 0.044715) * (a * a))
    return a * (0.5 + 0.5 * jnp.tanh(inner))


def kernel(cores, x_ref, ln1s_h, ln1b_h, win_h, bin_h, ln2s_h, ln2b_h, wsp_h, bsp_h, mask_h, wout_h, bout_h, out_ref,
           xbuf, u, hv, g, vn, wm, mask, win, wout, q, obuf, ln1s, ln1b, b_in, ln2s, ln2b, bsp, bout,
           small_sem, win_sem, wout_sem, wsp_sem, mask_sem, xs_sem, xr_sem, vs_sem, vr_sem, os_sem, or_sem):
    data, me = lax.axis_index("data"), lax.axis_index("seq")
    chip, core = me // cores, me % cores
    partner = (data, chip * cores + (cores - 1 - core))
    chips, rows, width = x_ref.shape
    gate = wout_h.shape[0]

    def block_of(k):
        return k * cores + core

    def row_slice(k):
        return pl.ds(pl.multiple_of(block_of(k) * rows, rows), rows)

    part = rows // HALVES

    def part_rows(half):
        return pl.ds(pl.multiple_of(half * part, part), part)

    for half in range(HALVES):
        rs = part_rows(half)
        pltpu.make_async_copy(x_ref.at[chip, rs], xbuf.at[chip, rs], xr_sem.at[chip * HALVES + half]).start()
    smalls = [pltpu.make_async_copy(src, dst, small_sem.at[i]) for i, (src, dst) in enumerate(
        ((ln1s_h, ln1s), (ln1b_h, ln1b), (bin_h, b_in), (ln2s_h, ln2s), (ln2b_h, ln2b), (bsp_h, bsp), (bout_h, bout)))]
    for cp in smalls:
        cp.start()
    win_v = pltpu.make_async_copy(win_h.at[:, pl.ds(gate, gate)], win.at[:, pl.ds(gate, gate)], win_sem.at[0])
    win_g = pltpu.make_async_copy(win_h.at[:, pl.ds(0, gate)], win.at[:, pl.ds(0, gate)], win_sem.at[1])
    win_v.start()
    win_g.start()

    barrier = pltpu.get_barrier_semaphore()
    pl.semaphore_signal(barrier, inc=1, device_id=partner, device_id_type=MESH)
    for d in range(1, chips):
        pl.semaphore_signal(barrier, inc=1, device_id=(data, (chip + d) % chips * cores + core), device_id_type=MESH)
    pl.semaphore_wait(barrier, chips)

    def x_copy(d, half):
        to = (chip + d) % chips
        rs = part_rows(half)
        return pltpu.make_async_remote_copy(
            src_ref=x_ref.at[to, rs], dst_ref=xbuf.at[chip, rs], send_sem=xs_sem.at[(d - 1) * HALVES + half],
            recv_sem=xr_sem.at[chip * HALVES + half], device_id=(data, to * cores + core), device_id_type=MESH)

    near = [d for d in range(1, chips) if d != chips // 2]
    for group in (near, [chips // 2]):
        for half in range(HALVES):
            for d in group:
                x_copy(d, half).start()

    spatial_loads = []
    for k in range(chips):
        cols = pl.ds(0, (k + 1) * cores * rows)
        spatial_loads += [
            pltpu.make_async_copy(wsp_h.at[row_slice(k), cols], wm.at[k, :, cols], wsp_sem.at[k]),
            pltpu.make_async_copy(mask_h.at[row_slice(k), cols], mask.at[k, :, cols], mask_sem.at[k]),
        ]
    wout_load = pltpu.make_async_copy(wout_h, wout, wout_sem)

    tile = gate // 4

    def dense(count, cols):
        a = jnp.dot(u[:count, :], win[:, cols], preferred_element_type=F32) + b_in[:, cols]
        return gelu(a).astype(BF16)

    def vn_copy(k, half):
        ws = pl.ds(pl.multiple_of(block_of(k) * rows + half * part, part), part)
        return pltpu.make_async_remote_copy(
            src_ref=vn.at[ws, :], dst_ref=vn.at[ws, :], send_sem=vs_sem.at[k * HALVES + half],
            recv_sem=vr_sem.at[k * HALVES + half], device_id=partner, device_id_type=MESH)

    def ln1(k, first, count):
        chunk = 32

        def body(r, carry):
            us = pl.ds(pl.multiple_of(r * chunk, chunk), chunk)
            xs = pl.ds(pl.multiple_of(first + r * chunk, chunk), chunk)
            u[us, :] = layer_norm_rows(xbuf[k, xs, :].astype(F32), ln1s[...], ln1b[...]).astype(BF16)
            return carry
        lax.fori_loop(0, count // chunk, body, 0, unroll=True)

    def values(count):
        def body(t, carry):
            start = pl.multiple_of(t * tile, tile)
            hv[:count, pl.ds(start, tile)] = dense(count, pl.ds(gate + start, tile))
            return carry
        lax.fori_loop(0, gate // tile, body, 0, unroll=True)

    chunk2 = 16

    def ln2(k, first, r):
        hs = pl.ds(pl.multiple_of(r * chunk2, chunk2), chunk2)
        ws = pl.ds(pl.multiple_of(block_of(k) * rows + first + r * chunk2, chunk2), chunk2)
        vn[ws, :] = layer_norm_rows(hv[hs, :].astype(F32), ln2s[...], ln2b[...]).astype(BF16)

    def ln2_all(k, first, count):
        def body(r, carry):
            ln2(k, first, r)
            return carry
        lax.fori_loop(0, count // chunk2, body, 0, unroll=True)

    def gates(k, first, count, with_ln2):
        per_tile = count // chunk2 // (gate // tile)
        gs = pl.ds(pl.multiple_of(first, count), count)

        def body(t, carry):
            cols = pl.ds(pl.multiple_of(t * tile, tile), tile)
            g[k, gs, cols] = dense(count, cols)
            if with_ln2:
                for r in range(per_tile):
                    ln2(k, first, t * per_tile + r)
            return carry
        lax.fori_loop(0, gate // tile, body, 0, unroll=True)

    def x_wait(k, half):
        rs = part_rows(half)
        pltpu.make_async_copy(xbuf.at[k, rs], xbuf.at[k, rs], xr_sem.at[k * HALVES + half]).wait()

    def do_own():
        for half in range(HALVES):
            x_wait(chip, half)
        for cp in smalls:
            cp.wait()
        ln1(chip, 0, rows)
        win_v.wait()
        for cp in spatial_loads:
            cp.start()
        values(rows)
        win_g.wait()
        wout_load.start()
        gates(chip, 0, rows, True)
        for half in range(HALVES):
            vn_copy(chip, half).start()

    def do_v(k, half):
        x_wait(k, half)
        first = half * part
        ln1(k, first, part)
        values(part)
        last = jnp.logical_and(k == (chip + chips // 2) % chips, half == HALVES - 1)

        @pl.when(last)
        def _():
            ln2_all(k, first, part)
            vn_copy(k, half).start()

        @pl.when(jnp.logical_not(last))
        def _():
            gates(k, first, part, True)
            vn_copy(k, half).start()

    def do_mask():
        for cp in spatial_loads:
            cp.wait()
        chunk = 32
        for k in range(chips):
            cols = slice(0, (k + 1) * cores * rows)

            def body(r, carry):
                rs = pl.ds(pl.multiple_of(r * chunk, chunk), chunk)
                keep = mask[k, rs, cols] > 0
                wm[k, rs, cols] = jnp.where(keep, wm[k, rs, cols].astype(F32), 0.0).astype(BF16)
                return carry
            lax.fori_loop(0, rows // chunk, body, 0)
        wout_load.wait()

    def out_copy(k, half):
        rs = part_rows(half)
        return pltpu.make_async_remote_copy(
            src_ref=obuf.at[k, rs], dst_ref=out_ref.at[chip, rs], send_sem=os_sem.at[k * HALVES + half],
            recv_sem=or_sem.at[chip * HALVES + half], device_id=(data, k * cores + core), device_id_type=MESH)

    def do_o(k, half):
        rs = part_rows(half)
        bias_row = bsp[:, pl.ds(pl.multiple_of(block_of(k) * rows + half * part, part), part)]
        bias = jnp.transpose(jnp.broadcast_to(bias_row, (128, part)))[:, :1]
        for kk in range(chips):
            @pl.when(k == kk)
            def _():
                depth = (kk + 1) * cores * rows

                def body(t, carry):
                    cols = pl.ds(pl.multiple_of(t * tile, tile), tile)
                    s = jnp.dot(wm[kk, rs, :depth], vn[:depth, cols], preferred_element_type=F32) + bias
                    q[:, cols] = (g[kk, rs, cols].astype(F32) * s.astype(BF16).astype(F32)).astype(BF16)
                    return carry
                lax.fori_loop(0, gate // tile, body, 0, unroll=True)
        out_tile = width // 2

        def out_body(t, carry):
            cols = pl.ds(pl.multiple_of(t * out_tile, out_tile), out_tile)
            y = jnp.dot(q[...], wout[:, cols], preferred_element_type=F32) + bout[:, cols]
            obuf[k, rs, cols] = (xbuf[k, rs, cols].astype(F32) + y).astype(BF16)
            return carry
        lax.fori_loop(0, width // out_tile, out_body, 0, unroll=True)

        @pl.when(k == chip)
        def _():
            pltpu.make_async_copy(obuf.at[k, rs], out_ref.at[chip, rs], or_sem.at[chip * HALVES + half]).start()

        @pl.when(k != chip)
        def _():
            out_copy(k, half).start()

    length = len(SCHEDULES[0])
    words = []
    for first in range(0, length, PER_WORD):
        word = jnp.int32(0)
        for c, steps in enumerate(SCHEDULES):
            word = jnp.where(chip == c, pack(steps[first:first + PER_WORD]), word)
        words.append(word)

    def step(i, carry):
        code = words[0]
        for n in range(1, len(words)):
            code = jnp.where(i >= n * PER_WORD, words[n], code)
        action = lax.shift_right_logical(code, BITS * (i % PER_WORD)) % (1 << BITS)

        @pl.when(action < W)
        def _():
            do_v(action // HALVES, action % HALVES)

        @pl.when(jnp.logical_and(action >= W, action < O_FIRST))
        def _():
            for half in range(HALVES):
                vn_copy(action - W, half).wait_recv()

        @pl.when(jnp.logical_and(action >= O_FIRST, action < G))
        def _():
            do_o((action - O_FIRST) // HALVES, action % HALVES)

        @pl.when(action == G)
        def _():
            gates((chip + chips // 2) % chips, (HALVES - 1) * part, part, False)
        return carry
    do_own()
    do_mask()
    lax.fori_loop(0, length, step, 0)

    for d in range(1, chips):
        for half in range(HALVES):
            x_copy(d, half).wait_send()
    for k in range(chips):
        for half in range(HALVES):
            vn_copy(k, half).wait_send()

        @pl.when(k != chip)
        def _():
            for half in range(HALVES):
                out_copy(k, half).wait_send()
    for k in range(chips):
        for half in range(HALVES):
            rs = part_rows(half)
            pltpu.make_async_copy(out_ref.at[k, rs], out_ref.at[k, rs], or_sem.at[k * HALVES + half]).wait()


def settle(src, dst, buf, in_sem, out_sem):
    count = src.shape[0]
    loads = [pltpu.make_async_copy(src.at[i], buf.at[i], in_sem.at[i]) for i in range(count)]
    stores = [pltpu.make_async_copy(buf.at[i], dst.at[i], out_sem.at[i]) for i in range(count)]
    for cp in loads:
        cp.start()
    for load, store in zip(loads, stores):
        load.wait()
        store.start()
    for cp in stores:
        cp.wait()


def solution(mesh):
    row_spec = P('data', 'seq', None)
    replicated = P()

    def local_block(act_in, ln1_scale, ln1_bias, w_in, b_in, ln2_scale, ln2_bias, w_spatial, b_spatial, causal_mask, w_out, b_out):
        chips, rows, width = act_in.shape
        cores = mesh.shape['seq'] // chips
        ffn, gate, total = w_in.shape[1], w_out.shape[0], w_spatial.shape[0]
        any_spec = pl.BlockSpec(memory_space=pl.ANY)
        row = lambda a: a.reshape(1, -1)
        dma = pltpu.SemaphoreType.DMA
        placed = pl.pallas_call(
            functools.partial(kernel, cores),
            out_shape=jax.ShapeDtypeStruct(act_in.shape, act_in.dtype),
            in_specs=[any_spec] * 12,
            out_specs=any_spec,
            scratch_shapes=[
                pltpu.VMEM((chips, rows, width), BF16),
                pltpu.VMEM((rows, width), BF16),
                pltpu.VMEM((rows, gate), BF16),
                pltpu.VMEM((chips, rows, gate), BF16),
                pltpu.VMEM((total, gate), BF16),
                pltpu.VMEM((chips, rows, total), BF16),
                pltpu.VMEM((chips, rows, total), jnp.int32),
                pltpu.VMEM((width, ffn), BF16),
                pltpu.VMEM((gate, width), BF16),
                pltpu.VMEM((rows // HALVES, gate), BF16),
                pltpu.VMEM((chips, rows, width), BF16),
                pltpu.VMEM((1, width), F32),
                pltpu.VMEM((1, width), F32),
                pltpu.VMEM((1, ffn), F32),
                pltpu.VMEM((1, gate), F32),
                pltpu.VMEM((1, gate), F32),
                pltpu.VMEM((1, total), F32),
                pltpu.VMEM((1, width), F32),
                dma((7,)), dma((2,)), dma, dma((chips,)), dma((chips,)),
                dma(((chips - 1) * HALVES,)), dma((chips * HALVES,)), dma((chips * HALVES,)), dma((chips * HALVES,)), dma((chips * HALVES,)), dma((chips * HALVES,)),
            ],
            compiler_params=pltpu.CompilerParams(collective_id=0, has_side_effects=True, vmem_limit_bytes=66_000_000),
        )(act_in, row(ln1_scale), row(ln1_bias), w_in, row(b_in), row(ln2_scale), row(ln2_bias), w_spatial, row(b_spatial),
          causal_mask, w_out, row(b_out))
        pieces = chips * HALVES
        piece = (pieces, rows // HALVES, width)
        return pl.pallas_call(
            settle,
            out_shape=jax.ShapeDtypeStruct(piece, act_in.dtype),
            in_specs=[any_spec],
            out_specs=any_spec,
            scratch_shapes=[pltpu.VMEM(piece, BF16), dma((pieces,)), dma((pieces,))],
        )(placed.reshape(piece)).reshape(act_in.shape)

    return jax.shard_map(local_block, mesh=mesh, in_specs=(row_spec,) + (replicated,) * 11, out_specs=row_spec, check_vma=False)
```

```python
import functools

import jax
import jax.numpy as jnp
from jax import lax
from jax.experimental import pallas as pl
from jax.experimental.pallas import tpu as pltpu
from jax.sharding import PartitionSpec as P

LN_EPS = 1e-6
MESH = pl.DeviceIdType.MESH
F32 = jnp.float32
BF16 = jnp.bfloat16

HALVES = 2
PIECES = 3


def V(k, half):
    return k * HALVES + half


def O(k, half):
    return 12 + k * HALVES + half


W, O_FIRST, G, PART, LEAD, BITS, PER_WORD = 8, 12, 20, 21, 22, 5, 6
SCHEDULES = (
    (V(1, 0), V(3, 0), V(1, 1), V(3, 1), V(2, 0), W + 0, W + 1, O(1, 0), V(2, 1), W + 3, PART, W + 2, LEAD,
     O(3, 1), O(1, 1), G, O(2, 0), O(2, 1), O(0, 0), O(0, 1)),
) * 2 + (
    (V(0, 0), V(2, 0), V(0, 1), V(2, 1), W + 0, W + 1, O(0, 0), O(0, 1), V(3, 0), W + 2, O(2, 0), O(2, 1), V(3, 1), PART, W + 3, LEAD,
     G, O(3, 1), O(1, 0), O(1, 1)),
) * 2 + (
    (V(1, 0), V(3, 0), V(1, 1), V(3, 1), V(0, 0), W + 1, PART, V(0, 1), G, W + 0, LEAD, O(0, 0), O(1, 1), O(0, 1), W + 2, W + 3,
     O(3, 0), O(3, 1), O(2, 0), O(2, 1)),
    (V(1, 0), V(3, 0), V(1, 1), V(3, 1), V(0, 0), W + 1, PART, V(0, 1), G, W + 0, O(0, 0), LEAD, O(0, 1), O(1, 1), W + 2, W + 3,
     O(3, 0), O(3, 1), O(2, 0), O(2, 1)),
) + (
    (V(0, 0), V(2, 0), V(0, 1), V(2, 1), W + 0, O(0, 0), O(0, 1), V(1, 0), PART, V(1, 1), G, W + 1, LEAD, W + 2, O(2, 0),
     O(1, 1), O(2, 1), W + 3, O(3, 0), O(3, 1)),
) * 2
LEADS = ((3, ((0, 2), (3, 4)), True), (3, ((0, 3),), True), (1, ((1, 2),), False), (1, ((0, 1),), False))


def pack(steps):
    return sum(s << (BITS * i) for i, s in enumerate(steps))


def layer_norm_rows(rows, gain, shift):
    mean = jnp.mean(rows, axis=-1, keepdims=True)
    centered = rows - mean
    var = jnp.mean(centered * centered, axis=-1, keepdims=True)
    return centered * lax.rsqrt(var + LN_EPS) * gain + shift


def gelu(a):
    c0 = 0.7978845608028654
    inner = a * (c0 + (c0 * 0.044715) * (a * a))
    return a * (0.5 + 0.5 * jnp.tanh(inner))


def kernel(cores, x_ref, ln1s_h, ln1b_h, win_h, bin_h, ln2s_h, ln2b_h, wsp_h, bsp_h, mask_h, wout_h, bout_h, out_ref,
           xbuf, u, hv, g, vn, wm, mask, win, wout, q, acc, obuf, ln1s, ln1b, b_in, ln2s, ln2b, bsp, bout,
           small_sem, win_sem, wout_sem, wsp_sem, mask_sem, xs_sem, xr_sem, vs_sem, vr_sem, os_sem, or_sem):
    data, me = lax.axis_index("data"), lax.axis_index("seq")
    chip, core = me // cores, me % cores
    other = cores - 1 - core
    partner = (data, chip * cores + other)
    chips, rows, width = x_ref.shape
    gate = wout_h.shape[0]

    def block_of(k):
        return k * cores + jnp.where(k == chip, core, other)

    def row_slice(k):
        return pl.ds(pl.multiple_of(block_of(k) * rows, rows), rows)

    barrier = pltpu.get_barrier_semaphore()
    for d in range(1, chips):
        pl.semaphore_signal(barrier, inc=1, device_id=(data, (chip + d) % chips * cores + other), device_id_type=MESH)
    pl.semaphore_signal(barrier, inc=1, device_id=partner, device_id_type=MESH)

    part = rows // HALVES
    far = (chip + chips // 2) % chips

    def part_rows(half):
        return pl.ds(pl.multiple_of(half * part, part), part)

    for half in range(HALVES):
        rs = part_rows(half)
        pltpu.make_async_copy(x_ref.at[chip, rs], xbuf.at[chip, rs], xr_sem.at[chip * HALVES + half]).start()
    smalls = [pltpu.make_async_copy(src, dst, small_sem.at[i]) for i, (src, dst) in enumerate(
        ((ln1s_h, ln1s), (ln1b_h, ln1b), (bin_h, b_in), (ln2s_h, ln2s), (ln2b_h, ln2b), (bsp_h, bsp), (bout_h, bout)))]
    for cp in smalls:
        cp.start()
    win_v = pltpu.make_async_copy(win_h.at[:, pl.ds(gate, gate)], win.at[:, pl.ds(gate, gate)], win_sem.at[0])
    win_g = pltpu.make_async_copy(win_h.at[:, pl.ds(0, gate)], win.at[:, pl.ds(0, gate)], win_sem.at[1])
    win_v.start()
    win_g.start()

    pl.semaphore_wait(barrier, chips)

    def x_copy(d, half):
        to = (chip + d) % chips
        rs = part_rows(half)
        return pltpu.make_async_remote_copy(
            src_ref=x_ref.at[to, rs], dst_ref=xbuf.at[chip, rs], send_sem=xs_sem.at[(d - 1) * HALVES + half],
            recv_sem=xr_sem.at[chip * HALVES + half], device_id=(data, to * cores + other), device_id_type=MESH)

    near = [d for d in range(1, chips) if d != chips // 2]
    for group in (near, [chips // 2]):
        for half in range(HALVES):
            for d in group:
                x_copy(d, half).start()

    spatial_loads = []
    for k in range(chips):
        cols = pl.ds(0, (k + 1) * cores * rows)
        spatial_loads += [
            pltpu.make_async_copy(wsp_h.at[row_slice(k), cols], wm.at[k, :, cols], wsp_sem.at[k]),
            pltpu.make_async_copy(mask_h.at[row_slice(k), cols], mask.at[k, :, cols], mask_sem.at[k]),
        ]
    wout_load = pltpu.make_async_copy(wout_h, wout, wout_sem)

    tile = gate // 4

    def dense(count, cols):
        a = jnp.dot(u[:count, :], win[:, cols], preferred_element_type=F32) + b_in[:, cols]
        return gelu(a).astype(BF16)

    def vn_copy(k, first, count, i):
        ws = pl.ds(pl.multiple_of(block_of(k) * rows + first, count), count)
        return pltpu.make_async_remote_copy(
            src_ref=vn.at[ws, :], dst_ref=vn.at[ws, :], send_sem=vs_sem.at[k * PIECES + i],
            recv_sem=vr_sem.at[k * PIECES + i], device_id=partner, device_id_type=MESH)

    def last_vn(i):
        return vn_copy(far, part + i * (part // 2), part // 2, 1 + i)

    def each_vn_copy(k, act):
        act(vn_copy(k, 0, part, 0))

        @pl.when(k != far)
        def _():
            act(vn_copy(k, part, part, 1))

        @pl.when(k == far)
        def _():
            for i in range(2):
                act(last_vn(i))

    def ln1(k, first, count):
        chunk = 32

        def body(r, carry):
            us = pl.ds(pl.multiple_of(r * chunk, chunk), chunk)
            xs = pl.ds(pl.multiple_of(first + r * chunk, chunk), chunk)
            u[us, :] = layer_norm_rows(xbuf[k, xs, :].astype(F32), ln1s[...], ln1b[...]).astype(BF16)
            return carry
        lax.fori_loop(0, count // chunk, body, 0, unroll=True)

    def values(count):
        def body(t, carry):
            start = pl.multiple_of(t * tile, tile)
            hv[:count, pl.ds(start, tile)] = dense(count, pl.ds(gate + start, tile))
            return carry
        lax.fori_loop(0, gate // tile, body, 0, unroll=True)

    chunk2 = 16

    def ln2(k, first, r):
        hs = pl.ds(pl.multiple_of(r * chunk2, chunk2), chunk2)
        ws = pl.ds(pl.multiple_of(block_of(k) * rows + first + r * chunk2, chunk2), chunk2)
        vn[ws, :] = layer_norm_rows(hv[hs, :].astype(F32), ln2s[...], ln2b[...]).astype(BF16)

    def ln2_last():
        each = part // 2 // chunk2
        for i in range(2):
            def body(r, carry):
                ln2(far, part, i * each + r)
                return carry
            lax.fori_loop(0, each, body, 0, unroll=True)
            last_vn(i).start()

    def gates(k, first, count, with_ln2):
        per_tile = count // chunk2 // (gate // tile)
        gs = pl.ds(pl.multiple_of(first, count), count)

        def body(t, carry):
            cols = pl.ds(pl.multiple_of(t * tile, tile), tile)
            g[k, gs, cols] = dense(count, cols)
            if with_ln2:
                for r in range(per_tile):
                    ln2(k, first, t * per_tile + r)
            return carry
        lax.fori_loop(0, gate // tile, body, 0, unroll=True)

    def x_wait(k, half):
        rs = part_rows(half)
        pltpu.make_async_copy(xbuf.at[k, rs], xbuf.at[k, rs], xr_sem.at[k * HALVES + half]).wait()

    def do_own():
        for half in range(HALVES):
            x_wait(chip, half)
        for cp in smalls:
            cp.wait()
        ln1(chip, 0, rows)
        win_v.wait()
        for cp in spatial_loads:
            cp.start()
        values(rows)
        win_g.wait()
        wout_load.start()
        gates(chip, 0, rows, True)
        each_vn_copy(chip, lambda cp: cp.start())

    def do_v(k, half):
        x_wait(k, half)
        first = half * part
        ln1(k, first, part)
        values(part)
        last = jnp.logical_and(k == far, half == HALVES - 1)

        @pl.when(last)
        def _():
            ln2_last()

        @pl.when(jnp.logical_not(last))
        def _():
            gates(k, first, part, True)
            for which in range(HALVES):
                @pl.when(half == which)
                def _():
                    vn_copy(k, which * part, part, which).start()

    def do_mask():
        for cp in spatial_loads:
            cp.wait()
        chunk = 32
        for k in range(chips):
            cols = slice(0, (k + 1) * cores * rows)

            def body(r, carry):
                rs = pl.ds(pl.multiple_of(r * chunk, chunk), chunk)
                keep = mask[k, rs, cols] > 0
                wm[k, rs, cols] = jnp.where(keep, wm[k, rs, cols].astype(F32), 0.0).astype(BF16)
                return carry
            lax.fori_loop(0, rows // chunk, body, 0)
        wout_load.wait()

    def out_copy(k, half):
        rs = part_rows(half)
        return pltpu.make_async_remote_copy(
            src_ref=obuf.at[k, rs], dst_ref=out_ref.at[chip, rs], send_sem=os_sem.at[k * HALVES + half],
            recv_sem=or_sem.at[chip * HALVES + half], device_id=(data, k * cores + other), device_id_type=MESH)

    def bias_of(k, half):
        bias_row = bsp[:, pl.ds(pl.multiple_of(block_of(k) * rows + half * part, part), part)]
        return jnp.transpose(jnp.broadcast_to(bias_row, (128, part)))[:, :1]

    def over_tiles(body):
        def step(t, carry):
            body(pl.ds(pl.multiple_of(t * tile, tile), tile))
            return carry
        lax.fori_loop(0, gate // tile, step, 0, unroll=True)

    def gated(k, rs, cols, s):
        return (g[k, rs, cols].astype(F32) * s.astype(BF16).astype(F32)).astype(BF16)

    def do_o(k, half):
        rs = part_rows(half)
        bias = bias_of(k, half)
        for kk in range(chips):
            @pl.when(k == kk)
            def _():
                depth = (kk + 1) * cores * rows

                def body(cols):
                    s = jnp.dot(wm[kk, rs, :depth], vn[:depth, cols], preferred_element_type=F32) + bias
                    q[:, cols] = gated(kk, rs, cols, s)
                over_tiles(body)
        finish_o(k, half)

    def do_part():
        own_block = pl.ds(pl.multiple_of((far * cores + other) * rows, rows), rows)
        for c, (k, spans, with_own) in enumerate(LEADS):
            @pl.when(chip == c)
            def _():
                def body(cols):
                    terms = [slice(first * cores * rows, end * cores * rows) for first, end in spans]
                    if with_own:
                        terms.append(own_block)
                    acc[:, cols] = sum(
                        jnp.dot(wm[k, :part, js], vn[js, cols], preferred_element_type=F32) for js in terms)
                over_tiles(body)

    def do_lead():
        k = lead
        bias = bias_of(k, 0)
        rs = pl.ds(0, part)

        def rest(js):
            def body(cols):
                s = jnp.dot(wm[k, rs, js], vn[js, cols], preferred_element_type=F32) + acc[:, cols] + bias
                q[:, cols] = gated(k, rs, cols, s)
            over_tiles(body)

        @pl.when(had_own)
        def _():
            rest(pl.ds(pl.multiple_of((far * cores + core) * rows, rows), rows))

        @pl.when(jnp.logical_not(had_own))
        def _():
            rest(pl.ds(pl.multiple_of(far * cores * rows, cores * rows), cores * rows))
        finish_o(k, 0)

    def finish_o(k, half):
        rs = part_rows(half)
        out_tile = width // 2

        def out_body(t, carry):
            cols = pl.ds(pl.multiple_of(t * out_tile, out_tile), out_tile)
            y = jnp.dot(q[...], wout[:, cols], preferred_element_type=F32) + bout[:, cols]
            obuf[k, rs, cols] = (xbuf[k, rs, cols].astype(F32) + y).astype(BF16)
            return carry
        lax.fori_loop(0, width // out_tile, out_body, 0, unroll=True)

        @pl.when(k == chip)
        def _():
            pltpu.make_async_copy(obuf.at[k, rs], out_ref.at[chip, rs], or_sem.at[chip * HALVES + half]).start()

        @pl.when(k != chip)
        def _():
            out_copy(k, half).start()

    lead, had_own = jnp.int32(0), False
    for c, (k, _, with_own) in enumerate(LEADS):
        lead = jnp.where(chip == c, k, lead)
        had_own = jnp.logical_or(had_own, jnp.logical_and(chip == c, with_own))
    length = len(SCHEDULES[0])
    words = []
    for first in range(0, length, PER_WORD):
        word = jnp.int32(0)
        for c, steps in enumerate(SCHEDULES):
            word = jnp.where(me == c, pack(steps[first:first + PER_WORD]), word)
        words.append(word)

    def step(i, carry):
        code = words[0]
        for n in range(1, len(words)):
            code = jnp.where(i >= n * PER_WORD, words[n], code)
        action = lax.shift_right_logical(code, BITS * (i % PER_WORD)) % (1 << BITS)

        @pl.when(action < W)
        def _():
            do_v(action // HALVES, action % HALVES)

        @pl.when(jnp.logical_and(action >= W, action < O_FIRST))
        def _():
            each_vn_copy(action - W, lambda cp: cp.wait_recv())

        @pl.when(jnp.logical_and(action >= O_FIRST, action < G))
        def _():
            do_o((action - O_FIRST) // HALVES, action % HALVES)

        @pl.when(action == G)
        def _():
            gates(far, (HALVES - 1) * part, part, False)

        @pl.when(action == PART)
        def _():
            do_part()

        @pl.when(action == LEAD)
        def _():
            do_lead()
        return carry
    do_own()
    do_mask()
    lax.fori_loop(0, length, step, 0)

    for d in range(1, chips):
        for half in range(HALVES):
            x_copy(d, half).wait_send()
    for k in range(chips):
        each_vn_copy(k, lambda cp: cp.wait_send())

        @pl.when(k != chip)
        def _():
            for half in range(HALVES):
                out_copy(k, half).wait_send()
    for k in range(chips):
        for half in range(HALVES):
            rs = part_rows(half)
            pltpu.make_async_copy(out_ref.at[k, rs], out_ref.at[k, rs], or_sem.at[k * HALVES + half]).wait()


def solution(mesh):
    row_spec = P('data', 'seq', None)
    replicated = P()

    def local_block(act_in, ln1_scale, ln1_bias, w_in, b_in, ln2_scale, ln2_bias, w_spatial, b_spatial, causal_mask, w_out, b_out):
        chips, rows, width = act_in.shape
        cores = mesh.shape['seq'] // chips
        ffn, gate, total = w_in.shape[1], w_out.shape[0], w_spatial.shape[0]
        any_spec = pl.BlockSpec(memory_space=pl.ANY)
        row = lambda a: a.reshape(1, -1)
        dma = pltpu.SemaphoreType.DMA
        return pl.pallas_call(
            functools.partial(kernel, cores),
            out_shape=pltpu.VMEM(act_in.shape, act_in.dtype),
            in_specs=[any_spec] * 12,
            out_specs=pl.BlockSpec(memory_space=pltpu.VMEM),
            scratch_shapes=[
                pltpu.VMEM((chips, rows, width), BF16),
                pltpu.VMEM((rows, width), BF16),
                pltpu.VMEM((rows, gate), BF16),
                pltpu.VMEM((chips, rows, gate), BF16),
                pltpu.VMEM((total, gate), BF16),
                pltpu.VMEM((chips, rows, total), BF16),
                pltpu.VMEM((chips, rows, total), jnp.int32),
                pltpu.VMEM((width, ffn), BF16),
                pltpu.VMEM((gate, width), BF16),
                pltpu.VMEM((rows // HALVES, gate), BF16),
                pltpu.VMEM((rows // HALVES, gate), F32),
                pltpu.VMEM((chips, rows, width), BF16),
                pltpu.VMEM((1, width), F32),
                pltpu.VMEM((1, width), F32),
                pltpu.VMEM((1, ffn), F32),
                pltpu.VMEM((1, gate), F32),
                pltpu.VMEM((1, gate), F32),
                pltpu.VMEM((1, total), F32),
                pltpu.VMEM((1, width), F32),
                dma((7,)), dma((2,)), dma, dma((chips,)), dma((chips,)),
                dma(((chips - 1) * HALVES,)), dma((chips * HALVES,)), dma((chips * PIECES,)), dma((chips * PIECES,)), dma((chips * HALVES,)), dma((chips * HALVES,)),
            ],
            compiler_params=pltpu.CompilerParams(collective_id=0, has_side_effects=True, vmem_limit_bytes=60_000_000),
        )(act_in, row(ln1_scale), row(ln1_bias), w_in, row(b_in), row(ln2_scale), row(ln2_bias), w_spatial, row(b_spatial),
          causal_mask, w_out, row(b_out))

    return jax.shard_map(local_block, mesh=mesh, in_specs=(row_spec,) + (replicated,) * 11, out_specs=row_spec, check_vma=False)
```

```python
import functools

import jax
import jax.numpy as jnp
from jax import lax
from jax.experimental import pallas as pl
from jax.experimental.pallas import tpu as pltpu
from jax.sharding import PartitionSpec as P

LN_EPS = 1e-6
MESH = pl.DeviceIdType.MESH
F32 = jnp.float32
BF16 = jnp.bfloat16

HALVES = 2
PIECES = 3


def V(k, half):
    return k * HALVES + half


def O(k, half):
    return 12 + k * HALVES + half


W, O_FIRST, G, PART, LEAD, OWN, LAST, NONE, BITS, PER_WORD = 8, 12, 20, 21, 22, 23, 24, 31, 5, 6
SCHEDULES = (
    (V(1, 0), V(3, 0), V(1, 1), V(3, 1), V(2, 0), W + 0, W + 1, O(1, 0), LAST, W + 3, PART, W + 2, LEAD,
     O(3, 1), O(1, 1), G, O(2, 0), O(2, 1), O(0, 0), O(0, 1)),
) * 2 + (
    (V(0, 0), V(2, 0), V(0, 1), V(2, 1), W + 0, W + 1, O(0, 0), O(0, 1), V(3, 0), W + 2, O(2, 0), O(2, 1), LAST, PART, W + 3, LEAD,
     G, O(3, 1), O(1, 0), O(1, 1)),
) * 2 + (
    (V(1, 0), V(3, 0), V(1, 1), V(3, 1), V(0, 0), W + 1, PART, LAST, G, OWN, W + 0, LEAD, O(0, 0), O(1, 1), O(0, 1), W + 2, W + 3,
     O(3, 0), O(3, 1), O(2, 0), O(2, 1)),
    (V(1, 0), V(3, 0), V(1, 1), V(3, 1), V(0, 0), W + 1, PART, LAST, G, OWN, W + 0, O(0, 0), LEAD, O(0, 1), O(1, 1), W + 2, W + 3,
     O(3, 0), O(3, 1), O(2, 0), O(2, 1)),
) + (
    (V(0, 0), V(2, 0), V(0, 1), V(2, 1), W + 0, O(0, 0), O(0, 1), V(1, 0), PART, LAST, G, OWN, W + 1, LEAD, W + 2, O(2, 0),
     O(1, 1), O(2, 1), W + 3, O(3, 0), O(3, 1)),
) * 2
LEADS = ((3, ((0, 2), (3, 4)), True), (3, ((0, 3),), True), (1, ((1, 2),), False), (1, ((0, 1),), False))


def pack(steps):
    return sum(steps[i] << (BITS * i) if i < len(steps) else NONE << (BITS * i) for i in range(PER_WORD))


def layer_norm_rows(rows, gain, shift):
    mean = jnp.mean(rows, axis=-1, keepdims=True)
    centered = rows - mean
    var = jnp.mean(centered * centered, axis=-1, keepdims=True)
    return centered * lax.rsqrt(var + LN_EPS) * gain + shift


def gelu(a):
    c0 = 0.7978845608028654
    inner = a * (c0 + (c0 * 0.044715) * (a * a))
    return a * (0.5 + 0.5 * jnp.tanh(inner))


def kernel(cores, x_ref, ln1s_h, ln1b_h, win_h, bin_h, ln2s_h, ln2b_h, wsp_h, bsp_h, mask_h, wout_h, bout_h, out_ref,
           xbuf, u, hv, g, vn, wm, mask, win, wout, q, acc, obuf, ln1s, ln1b, b_in, ln2s, ln2b, bsp, bout,
           small_sem, win_sem, wout_sem, wsp_sem, mask_sem, xs_sem, xr_sem, vs_sem, vr_sem, os_sem, or_sem):
    data, me = lax.axis_index("data"), lax.axis_index("seq")
    chip, core = me // cores, me % cores
    other = cores - 1 - core
    partner = (data, chip * cores + other)
    chips, rows, width = x_ref.shape
    gate = wout_h.shape[0]

    def block_of(k):
        return k * cores + jnp.where(k == chip, core, other)

    def row_slice(k):
        return pl.ds(pl.multiple_of(block_of(k) * rows, rows), rows)

    barrier = pltpu.get_barrier_semaphore()
    for d in range(1, chips):
        pl.semaphore_signal(barrier, inc=1, device_id=(data, (chip + d) % chips * cores + other), device_id_type=MESH)
    pl.semaphore_signal(barrier, inc=1, device_id=partner, device_id_type=MESH)

    part = rows // HALVES
    far = (chip + chips // 2) % chips

    def part_rows(half):
        return pl.ds(pl.multiple_of(half * part, part), part)

    for half in range(HALVES):
        rs = part_rows(half)
        pltpu.make_async_copy(x_ref.at[chip, rs], xbuf.at[chip, rs], xr_sem.at[chip * HALVES + half]).start()
    smalls = [pltpu.make_async_copy(src, dst, small_sem.at[i]) for i, (src, dst) in enumerate(
        ((ln1s_h, ln1s), (ln1b_h, ln1b), (bin_h, b_in), (ln2s_h, ln2s), (ln2b_h, ln2b), (bsp_h, bsp), (bout_h, bout)))]
    for cp in smalls:
        cp.start()
    win_v = pltpu.make_async_copy(win_h.at[:, pl.ds(gate, gate)], win.at[:, pl.ds(gate, gate)], win_sem.at[0])
    win_g = pltpu.make_async_copy(win_h.at[:, pl.ds(0, gate)], win.at[:, pl.ds(0, gate)], win_sem.at[1])
    win_v.start()
    win_g.start()

    pl.semaphore_wait(barrier, chips)

    def x_copy(d, half):
        to = (chip + d) % chips
        rs = part_rows(half)
        return pltpu.make_async_remote_copy(
            src_ref=x_ref.at[to, rs], dst_ref=xbuf.at[chip, rs], send_sem=xs_sem.at[(d - 1) * HALVES + half],
            recv_sem=xr_sem.at[chip * HALVES + half], device_id=(data, to * cores + other), device_id_type=MESH)

    near = [d for d in range(1, chips) if d != chips // 2]
    for group in (near, [chips // 2]):
        for half in range(HALVES):
            for d in group:
                x_copy(d, half).start()

    spatial_loads = []
    for k in range(chips):
        cols = pl.ds(0, (k + 1) * cores * rows)
        spatial_loads += [
            pltpu.make_async_copy(wsp_h.at[row_slice(k), cols], wm.at[k, :, cols], wsp_sem.at[k]),
            pltpu.make_async_copy(mask_h.at[row_slice(k), cols], mask.at[k, :, cols], mask_sem.at[k]),
        ]
    wout_load = pltpu.make_async_copy(wout_h, wout, wout_sem)

    tile = gate // 4

    def dense(count, cols):
        a = jnp.dot(u[:count, :], win[:, cols], preferred_element_type=F32) + b_in[:, cols]
        return gelu(a).astype(BF16)

    def vn_copy(k, first, count, i):
        ws = pl.ds(pl.multiple_of(block_of(k) * rows + first, count), count)
        return pltpu.make_async_remote_copy(
            src_ref=vn.at[ws, :], dst_ref=vn.at[ws, :], send_sem=vs_sem.at[k * PIECES + i],
            recv_sem=vr_sem.at[k * PIECES + i], device_id=partner, device_id_type=MESH)

    def last_vn(i):
        return vn_copy(far, part + i * (part // 2), part // 2, 1 + i)

    def each_vn_copy(k, act):
        act(vn_copy(k, 0, part, 0))

        @pl.when(k != far)
        def _():
            act(vn_copy(k, part, part, 1))

        @pl.when(k == far)
        def _():
            for i in range(2):
                act(last_vn(i))

    def ln1(k, first, count):
        chunk = 32

        def body(r, carry):
            us = pl.ds(pl.multiple_of(r * chunk, chunk), chunk)
            xs = pl.ds(pl.multiple_of(first + r * chunk, chunk), chunk)
            u[us, :] = layer_norm_rows(xbuf[k, xs, :].astype(F32), ln1s[...], ln1b[...]).astype(BF16)
            return carry
        lax.fori_loop(0, count // chunk, body, 0, unroll=True)

    def values(count):
        def body(t, carry):
            start = pl.multiple_of(t * tile, tile)
            hv[:count, pl.ds(start, tile)] = dense(count, pl.ds(gate + start, tile))
            return carry
        lax.fori_loop(0, gate // tile, body, 0, unroll=True)

    chunk2 = 16

    def ln2(k, first, r):
        hs = pl.ds(pl.multiple_of(r * chunk2, chunk2), chunk2)
        ws = pl.ds(pl.multiple_of(block_of(k) * rows + first + r * chunk2, chunk2), chunk2)
        vn[ws, :] = layer_norm_rows(hv[hs, :].astype(F32), ln2s[...], ln2b[...]).astype(BF16)

    def ln2_last():
        each = part // 2 // chunk2
        for i in range(2):
            def body(r, carry):
                ln2(far, part, i * each + r)
                return carry
            lax.fori_loop(0, each, body, 0, unroll=True)
            last_vn(i).start()

    def gates(k, first, count, with_ln2):
        per_tile = count // chunk2 // (gate // tile)
        gs = pl.ds(pl.multiple_of(first, count), count)

        def body(t, carry):
            cols = pl.ds(pl.multiple_of(t * tile, tile), tile)
            g[k, gs, cols] = dense(count, cols)
            if with_ln2:
                for r in range(per_tile):
                    ln2(k, first, t * per_tile + r)
            return carry
        lax.fori_loop(0, gate // tile, body, 0, unroll=True)

    def x_wait(k, half):
        rs = part_rows(half)
        pltpu.make_async_copy(xbuf.at[k, rs], xbuf.at[k, rs], xr_sem.at[k * HALVES + half]).wait()

    def do_own():
        for half in range(HALVES):
            x_wait(chip, half)
        for cp in smalls:
            cp.wait()
        ln1(chip, 0, rows)
        win_v.wait()
        for cp in spatial_loads:
            cp.start()
        values(rows)
        win_g.wait()
        wout_load.start()
        gates(chip, 0, rows, True)
        each_vn_copy(chip, lambda cp: cp.start())

    def do_v(k, half):
        x_wait(k, half)
        first = half * part
        ln1(k, first, part)
        values(part)
        gates(k, first, part, True)
        for which in range(HALVES):
            @pl.when(half == which)
            def _():
                vn_copy(k, which * part, part, which).start()

    def do_last():
        x_wait(far, HALVES - 1)
        ln1(far, part, part)
        values(part)
        ln2_last()

    def do_mask():
        for cp in spatial_loads:
            cp.wait()
        chunk = 32
        for k in range(chips):
            cols = slice(0, (k + 1) * cores * rows)

            def body(r, carry):
                rs = pl.ds(pl.multiple_of(r * chunk, chunk), chunk)
                keep = mask[k, rs, cols] > 0
                wm[k, rs, cols] = jnp.where(keep, wm[k, rs, cols].astype(F32), 0.0).astype(BF16)
                return carry
            lax.fori_loop(0, rows // chunk, body, 0)
        wout_load.wait()

    def out_copy(k, half):
        rs = part_rows(half)
        return pltpu.make_async_remote_copy(
            src_ref=obuf.at[k, rs], dst_ref=out_ref.at[chip, rs], send_sem=os_sem.at[k * HALVES + half],
            recv_sem=or_sem.at[chip * HALVES + half], device_id=(data, k * cores + other), device_id_type=MESH)

    def bias_of(k, half):
        bias_row = bsp[:, pl.ds(pl.multiple_of(block_of(k) * rows + half * part, part), part)]
        return jnp.transpose(jnp.broadcast_to(bias_row, (128, part)))[:, :1]

    def over_tiles(body):
        def step(t, carry):
            body(pl.ds(pl.multiple_of(t * tile, tile), tile))
            return carry
        lax.fori_loop(0, gate // tile, step, 0, unroll=True)

    def gated(k, rs, cols, s):
        return (g[k, rs, cols].astype(F32) * s.astype(BF16).astype(F32)).astype(BF16)

    def do_o(k, half):
        rs = part_rows(half)
        bias = bias_of(k, half)
        for kk in range(chips):
            @pl.when(k == kk)
            def _():
                depth = (kk + 1) * cores * rows

                def body(cols):
                    s = jnp.dot(wm[kk, rs, :depth], vn[:depth, cols], preferred_element_type=F32) + bias
                    q[:, cols] = gated(kk, rs, cols, s)
                over_tiles(body)
        finish_o(k, half)

    def do_part():
        own_block = pl.ds(pl.multiple_of((far * cores + other) * rows, rows), rows)
        for c, (k, spans, with_own) in enumerate(LEADS):
            @pl.when(chip == c)
            def _():
                def body(cols):
                    terms = [slice(first * cores * rows, end * cores * rows) for first, end in spans]
                    if with_own:
                        terms.append(own_block)
                    acc[:, cols] = sum(
                        jnp.dot(wm[k, :part, js], vn[js, cols], preferred_element_type=F32) for js in terms)
                over_tiles(body)

    def do_lead():
        k = lead
        bias = bias_of(k, 0)
        rs = pl.ds(0, part)

        last_block = pl.ds(pl.multiple_of((far * cores + core) * rows, rows), rows)

        def body(cols):
            s = jnp.dot(wm[k, rs, last_block], vn[last_block, cols], preferred_element_type=F32) + acc[:, cols] + bias
            q[:, cols] = gated(k, rs, cols, s)
        over_tiles(body)
        finish_o(k, 0)

    def do_own_term():
        own_block = pl.ds(pl.multiple_of((far * cores + other) * rows, rows), rows)

        def body(cols):
            acc[:, cols] += jnp.dot(wm[lead, :part, own_block], vn[own_block, cols], preferred_element_type=F32)
        over_tiles(body)

    def finish_o(k, half):
        rs = part_rows(half)
        out_tile = width // 2

        def out_body(t, carry):
            cols = pl.ds(pl.multiple_of(t * out_tile, out_tile), out_tile)
            y = jnp.dot(q[...], wout[:, cols], preferred_element_type=F32) + bout[:, cols]
            obuf[k, rs, cols] = (xbuf[k, rs, cols].astype(F32) + y).astype(BF16)
            return carry
        lax.fori_loop(0, width // out_tile, out_body, 0, unroll=True)

        @pl.when(k == chip)
        def _():
            pltpu.make_async_copy(obuf.at[k, rs], out_ref.at[chip, rs], or_sem.at[chip * HALVES + half]).start()

        @pl.when(k != chip)
        def _():
            out_copy(k, half).start()

    lead = jnp.int32(0)
    for c, (k, _, _) in enumerate(LEADS):
        lead = jnp.where(chip == c, k, lead)
    length = max(len(steps) for steps in SCHEDULES)
    words = []
    for first in range(0, length, PER_WORD):
        word = jnp.int32(0)
        for c, steps in enumerate(SCHEDULES):
            word = jnp.where(me == c, pack(steps[first:first + PER_WORD]), word)
        words.append(word)

    def step(i, carry):
        code = words[0]
        for n in range(1, len(words)):
            code = jnp.where(i >= n * PER_WORD, words[n], code)
        action = lax.shift_right_logical(code, BITS * (i % PER_WORD)) % (1 << BITS)

        @pl.when(action < W)
        def _():
            do_v(action // HALVES, action % HALVES)

        @pl.when(jnp.logical_and(action >= W, action < O_FIRST))
        def _():
            each_vn_copy(action - W, lambda cp: cp.wait_recv())

        @pl.when(jnp.logical_and(action >= O_FIRST, action < G))
        def _():
            do_o((action - O_FIRST) // HALVES, action % HALVES)

        @pl.when(action == G)
        def _():
            gates(far, (HALVES - 1) * part, part, False)

        @pl.when(action == PART)
        def _():
            do_part()

        @pl.when(action == LEAD)
        def _():
            do_lead()

        @pl.when(action == OWN)
        def _():
            do_own_term()

        @pl.when(action == LAST)
        def _():
            do_last()
        return carry
    do_own()
    do_mask()
    lax.fori_loop(0, length, step, 0)

    for d in range(1, chips):
        for half in range(HALVES):
            x_copy(d, half).wait_send()
    for k in range(chips):
        each_vn_copy(k, lambda cp: cp.wait_send())

        @pl.when(k != chip)
        def _():
            for half in range(HALVES):
                out_copy(k, half).wait_send()
    for k in range(chips):
        for half in range(HALVES):
            rs = part_rows(half)
            pltpu.make_async_copy(out_ref.at[k, rs], out_ref.at[k, rs], or_sem.at[k * HALVES + half]).wait()


def solution(mesh):
    row_spec = P('data', 'seq', None)
    replicated = P()

    def local_block(act_in, ln1_scale, ln1_bias, w_in, b_in, ln2_scale, ln2_bias, w_spatial, b_spatial, causal_mask, w_out, b_out):
        chips, rows, width = act_in.shape
        cores = mesh.shape['seq'] // chips
        ffn, gate, total = w_in.shape[1], w_out.shape[0], w_spatial.shape[0]
        any_spec = pl.BlockSpec(memory_space=pl.ANY)
        row = lambda a: a.reshape(1, -1)
        dma = pltpu.SemaphoreType.DMA
        return pl.pallas_call(
            functools.partial(kernel, cores),
            out_shape=pltpu.VMEM(act_in.shape, act_in.dtype),
            in_specs=[any_spec] * 12,
            out_specs=pl.BlockSpec(memory_space=pltpu.VMEM),
            scratch_shapes=[
                pltpu.VMEM((chips, rows, width), BF16),
                pltpu.VMEM((rows, width), BF16),
                pltpu.VMEM((rows, gate), BF16),
                pltpu.VMEM((chips, rows, gate), BF16),
                pltpu.VMEM((total, gate), BF16),
                pltpu.VMEM((chips, rows, total), BF16),
                pltpu.VMEM((chips, rows, total), jnp.int32),
                pltpu.VMEM((width, ffn), BF16),
                pltpu.VMEM((gate, width), BF16),
                pltpu.VMEM((rows // HALVES, gate), BF16),
                pltpu.VMEM((rows // HALVES, gate), F32),
                pltpu.VMEM((chips, rows, width), BF16),
                pltpu.VMEM((1, width), F32),
                pltpu.VMEM((1, width), F32),
                pltpu.VMEM((1, ffn), F32),
                pltpu.VMEM((1, gate), F32),
                pltpu.VMEM((1, gate), F32),
                pltpu.VMEM((1, total), F32),
                pltpu.VMEM((1, width), F32),
                dma((7,)), dma((2,)), dma, dma((chips,)), dma((chips,)),
                dma(((chips - 1) * HALVES,)), dma((chips * HALVES,)), dma((chips * PIECES,)), dma((chips * PIECES,)), dma((chips * HALVES,)), dma((chips * HALVES,)),
            ],
            compiler_params=pltpu.CompilerParams(collective_id=0, has_side_effects=True, vmem_limit_bytes=60_000_000),
        )(act_in, row(ln1_scale), row(ln1_bias), w_in, row(b_in), row(ln2_scale), row(ln2_bias), w_spatial, row(b_spatial),
          causal_mask, w_out, row(b_out))

    return jax.shard_map(local_block, mesh=mesh, in_specs=(row_spec,) + (replicated,) * 11, out_specs=row_spec, check_vma=False)
```

```python
import functools

import jax
import jax.numpy as jnp
from jax import lax
from jax.experimental import pallas as pl
from jax.experimental.pallas import tpu as pltpu
from jax.sharding import PartitionSpec as P

LN_EPS = 1e-6
MESH = pl.DeviceIdType.MESH
F32 = jnp.float32
BF16 = jnp.bfloat16

HALVES = 2
PIECES = 3


def V(k, half):
    return k * HALVES + half


def O(k, half):
    return 12 + k * HALVES + half


W, O_FIRST, G, PART, LEAD, OWN, LAST, NONE, BITS, PER_WORD = 8, 12, 20, 21, 22, 23, 24, 31, 5, 6
SCHEDULES = (
    (V(1, 0), V(3, 0), V(1, 1), V(3, 1), V(2, 0), W + 0, W + 1, O(1, 0), LAST, W + 3, PART, W + 2, LEAD,
     O(3, 1), O(1, 1), G, O(2, 0), O(2, 1), O(0, 0), O(0, 1)),
) * 2 + (
    (V(0, 0), V(2, 0), V(0, 1), V(2, 1), W + 0, W + 1, O(0, 0), O(0, 1), V(3, 0), W + 2, O(2, 0), O(2, 1), LAST, PART, W + 3, LEAD,
     G, O(3, 1), O(1, 0), O(1, 1)),
) * 2 + (
    (V(1, 0), V(3, 0), V(1, 1), V(3, 1), V(0, 0), W + 1, PART, LAST, G, OWN, W + 0, LEAD, O(0, 0), O(1, 1), O(0, 1), W + 2, W + 3,
     O(3, 0), O(3, 1), O(2, 0), O(2, 1)),
    (V(1, 0), V(3, 0), V(1, 1), V(3, 1), V(0, 0), W + 1, PART, LAST, G, OWN, W + 0, O(0, 0), LEAD, O(0, 1), O(1, 1), W + 2, W + 3,
     O(3, 0), O(3, 1), O(2, 0), O(2, 1)),
) + (
    (V(0, 0), V(2, 0), V(0, 1), V(2, 1), W + 0, O(0, 0), O(0, 1), V(1, 0), PART, LAST, G, OWN, W + 1, LEAD, W + 2, O(2, 0),
     O(1, 1), O(2, 1), W + 3, O(3, 0), O(3, 1)),
) * 2
LEADS = ((3, ((0, 2), (3, 4)), True), (3, ((0, 3),), True), (1, ((1, 2),), False), (1, ((0, 1),), False))


def pack(steps):
    return sum(steps[i] << (BITS * i) if i < len(steps) else NONE << (BITS * i) for i in range(PER_WORD))


def layer_norm_rows(rows, gain, shift):
    mean = jnp.mean(rows, axis=-1, keepdims=True)
    centered = rows - mean
    var = jnp.mean(centered * centered, axis=-1, keepdims=True)
    return centered * lax.rsqrt(var + LN_EPS) * gain + shift


def gelu(a):
    c0 = 0.7978845608028654
    inner = a * (c0 + (c0 * 0.044715) * (a * a))
    return a * (0.5 + 0.5 * jnp.tanh(inner))


def kernel(cores, x_ref, ln1s_h, ln1b_h, win_h, bin_h, ln2s_h, ln2b_h, wsp_h, bsp_h, mask_h, wout_h, bout_h, out_ref,
           xbuf, u, hv, g, vn, wm, mask, win, wout, q, acc, obuf, ln1s, ln1b, b_in, ln2s, ln2b, bsp, bout,
           small_sem, win_sem, wout_sem, wsp_sem, mask_sem, xs_sem, xr_sem, vs_sem, vr_sem, os_sem, or_sem):
    data, me = lax.axis_index("data"), lax.axis_index("seq")
    chip, core = me // cores, me % cores
    other = cores - 1 - core
    partner = (data, chip * cores + other)
    chips, rows, width = x_ref.shape
    gate = wout_h.shape[0]

    def block_of(k):
        return k * cores + jnp.where(k == chip, core, other)

    def row_slice(k):
        return pl.ds(pl.multiple_of(block_of(k) * rows, rows), rows)

    barrier = pltpu.get_barrier_semaphore()
    for d in range(1, chips):
        pl.semaphore_signal(barrier, inc=1, device_id=(data, (chip + d) % chips * cores + other), device_id_type=MESH)
    pl.semaphore_signal(barrier, inc=1, device_id=partner, device_id_type=MESH)

    part = rows // HALVES
    far = (chip + chips // 2) % chips

    def part_rows(half):
        return pl.ds(pl.multiple_of(half * part, part), part)

    for half in range(HALVES):
        rs = part_rows(half)
        pltpu.make_async_copy(x_ref.at[chip, rs], xbuf.at[chip, rs], xr_sem.at[chip * HALVES + half]).start()
    smalls = [pltpu.make_async_copy(src, dst, small_sem.at[i]) for i, (src, dst) in enumerate(
        ((ln1s_h, ln1s), (ln1b_h, ln1b), (bin_h, b_in), (ln2s_h, ln2s), (ln2b_h, ln2b), (bsp_h, bsp), (bout_h, bout)))]
    for cp in smalls:
        cp.start()
    win_v = pltpu.make_async_copy(win_h.at[:, pl.ds(gate, gate)], win.at[:, pl.ds(gate, gate)], win_sem.at[0])
    win_g = pltpu.make_async_copy(win_h.at[:, pl.ds(0, gate)], win.at[:, pl.ds(0, gate)], win_sem.at[1])
    win_v.start()
    win_g.start()

    pl.semaphore_wait(barrier, chips)

    def x_copy(d, half):
        to = (chip + d) % chips
        rs = part_rows(half)
        return pltpu.make_async_remote_copy(
            src_ref=x_ref.at[to, rs], dst_ref=xbuf.at[chip, rs], send_sem=xs_sem.at[(d - 1) * HALVES + half],
            recv_sem=xr_sem.at[chip * HALVES + half], device_id=(data, to * cores + other), device_id_type=MESH)

    near = [d for d in range(1, chips) if d != chips // 2]
    for group in (near, [chips // 2]):
        for half in range(HALVES):
            for d in group:
                x_copy(d, half).start()

    spatial_loads = []
    for k in range(chips):
        cols = pl.ds(0, (k + 1) * cores * rows)
        spatial_loads += [
            pltpu.make_async_copy(wsp_h.at[row_slice(k), cols], wm.at[k, :, cols], wsp_sem.at[k]),
            pltpu.make_async_copy(mask_h.at[row_slice(k), cols], mask.at[k, :, cols], mask_sem.at[k]),
        ]
    wout_load = pltpu.make_async_copy(wout_h, wout, wout_sem)

    tile = gate // 4

    def dense(count, cols):
        a = jnp.dot(u[:count, :], win[:, cols], preferred_element_type=F32) + b_in[:, cols]
        return gelu(a).astype(BF16)

    def vn_copy(k, first, count, i):
        ws = pl.ds(pl.multiple_of(block_of(k) * rows + first, count), count)
        return pltpu.make_async_remote_copy(
            src_ref=vn.at[ws, :], dst_ref=vn.at[ws, :], send_sem=vs_sem.at[k * PIECES + i],
            recv_sem=vr_sem.at[k * PIECES + i], device_id=partner, device_id_type=MESH)

    def last_vn(i):
        return vn_copy(far, part + i * (part // 2), part // 2, 1 + i)

    def each_vn_copy(k, act):
        act(vn_copy(k, 0, part, 0))

        @pl.when(k != far)
        def _():
            act(vn_copy(k, part, part, 1))

        @pl.when(k == far)
        def _():
            for i in range(2):
                act(last_vn(i))

    def ln1(k, first, count):
        chunk = 32

        def body(r, carry):
            us = pl.ds(pl.multiple_of(r * chunk, chunk), chunk)
            xs = pl.ds(pl.multiple_of(first + r * chunk, chunk), chunk)
            u[us, :] = layer_norm_rows(xbuf[k, xs, :].astype(F32), ln1s[...], ln1b[...]).astype(BF16)
            return carry
        lax.fori_loop(0, count // chunk, body, 0, unroll=True)

    def values(count):
        def body(t, carry):
            start = pl.multiple_of(t * tile, tile)
            hv[:count, pl.ds(start, tile)] = dense(count, pl.ds(gate + start, tile))
            return carry
        lax.fori_loop(0, gate // tile, body, 0, unroll=True)

    chunk2 = 16

    def ln2(k, first, r):
        hs = pl.ds(pl.multiple_of(r * chunk2, chunk2), chunk2)
        ws = pl.ds(pl.multiple_of(block_of(k) * rows + first + r * chunk2, chunk2), chunk2)
        vn[ws, :] = layer_norm_rows(hv[hs, :].astype(F32), ln2s[...], ln2b[...]).astype(BF16)

    def ln2_last():
        each = part // 2 // chunk2
        for i in range(2):
            def body(r, carry):
                ln2(far, part, i * each + r)
                return carry
            lax.fori_loop(0, each, body, 0, unroll=True)
            last_vn(i).start()

    def gates(k, first, count, with_ln2):
        per_tile = count // chunk2 // (gate // tile)
        gs = pl.ds(pl.multiple_of(first, count), count)

        def body(t, carry):
            cols = pl.ds(pl.multiple_of(t * tile, tile), tile)
            g[k, gs, cols] = dense(count, cols)
            if with_ln2:
                for r in range(per_tile):
                    ln2(k, first, t * per_tile + r)
            return carry
        lax.fori_loop(0, gate // tile, body, 0, unroll=True)

    def x_wait(k, half):
        rs = part_rows(half)
        pltpu.make_async_copy(xbuf.at[k, rs], xbuf.at[k, rs], xr_sem.at[k * HALVES + half]).wait()

    def do_own():
        for half in range(HALVES):
            x_wait(chip, half)
        for cp in smalls:
            cp.wait()
        ln1(chip, 0, rows)
        win_v.wait()
        for cp in spatial_loads:
            cp.start()
        values(rows)
        win_g.wait()
        wout_load.start()
        gates(chip, 0, rows, True)
        each_vn_copy(chip, lambda cp: cp.start())

    def do_v(k, half):
        x_wait(k, half)
        first = half * part
        ln1(k, first, part)
        values(part)
        gates(k, first, part, True)
        for which in range(HALVES):
            @pl.when(half == which)
            def _():
                vn_copy(k, which * part, part, which).start()

    def do_last():
        x_wait(far, HALVES - 1)
        ln1(far, part, part)
        values(part)
        ln2_last()

    def do_mask():
        for cp in spatial_loads:
            cp.wait()
        chunk = 32
        for k in range(chips):
            cols = slice(0, (k + 1) * cores * rows)

            def body(r, carry):
                rs = pl.ds(pl.multiple_of(r * chunk, chunk), chunk)
                keep = mask[k, rs, cols] > 0
                wm[k, rs, cols] = jnp.where(keep, wm[k, rs, cols].astype(F32), 0.0).astype(BF16)
                return carry
            lax.fori_loop(0, rows // chunk, body, 0)
        wout_load.wait()

    def out_copy(k, half):
        rs = part_rows(half)
        return pltpu.make_async_remote_copy(
            src_ref=obuf.at[k, rs], dst_ref=out_ref.at[chip, rs], send_sem=os_sem.at[k * HALVES + half],
            recv_sem=or_sem.at[chip * HALVES + half], device_id=(data, k * cores + other), device_id_type=MESH)

    def bias_of(k, half):
        bias_row = bsp[:, pl.ds(pl.multiple_of(block_of(k) * rows + half * part, part), part)]
        return jnp.transpose(jnp.broadcast_to(bias_row, (128, part)))[:, :1]

    def over_tiles(body):
        def step(t, carry):
            body(pl.ds(pl.multiple_of(t * tile, tile), tile))
            return carry
        lax.fori_loop(0, gate // tile, step, 0, unroll=True)

    def gated(k, rs, cols, s):
        return (g[k, rs, cols].astype(F32) * s.astype(BF16).astype(F32)).astype(BF16)

    def do_o(k, half):
        rs = part_rows(half)
        bias = bias_of(k, half)
        for kk in range(chips):
            @pl.when(k == kk)
            def _():
                depth = (kk + 1) * cores * rows

                def body(cols):
                    s = jnp.dot(wm[kk, rs, :depth], vn[:depth, cols], preferred_element_type=F32) + bias
                    q[:, cols] = gated(kk, rs, cols, s)
                over_tiles(body)
        finish_o(k, half)

    def do_part():
        own_block = pl.ds(pl.multiple_of((far * cores + other) * rows, rows), rows)
        for c, (k, spans, with_own) in enumerate(LEADS):
            @pl.when(chip == c)
            def _():
                def body(cols):
                    terms = [slice(first * cores * rows, end * cores * rows) for first, end in spans]
                    if with_own:
                        terms.append(own_block)
                    acc[:, cols] = sum(
                        jnp.dot(wm[k, :part, js], vn[js, cols], preferred_element_type=F32) for js in terms)
                over_tiles(body)

    def do_lead():
        k = lead
        bias = bias_of(k, 0)
        rs = pl.ds(0, part)

        last_block = pl.ds(pl.multiple_of((far * cores + core) * rows, rows), rows)

        def body(cols):
            s = jnp.dot(wm[k, rs, last_block], vn[last_block, cols], preferred_element_type=F32) + acc[:, cols] + bias
            q[:, cols] = gated(k, rs, cols, s)
        over_tiles(body)
        for t in range(2):
            cs = slice(t * (width // 2), (t + 1) * (width // 2))
            y = jnp.dot(q[...], wout[:, cs], preferred_element_type=F32) + bout[:, cs]
            obuf[k, rs, cs] = (xbuf[k, rs, cs].astype(F32) + y).astype(BF16)
            pltpu.make_async_remote_copy(
                src_ref=obuf.at[k, rs, cs], dst_ref=out_ref.at[chip, rs, cs], send_sem=os_sem.at[k * HALVES],
                recv_sem=or_sem.at[chip * HALVES], device_id=(data, k * cores + other), device_id_type=MESH).start()

    def do_own_term():
        own_block = pl.ds(pl.multiple_of((far * cores + other) * rows, rows), rows)

        def body(cols):
            acc[:, cols] += jnp.dot(wm[lead, :part, own_block], vn[own_block, cols], preferred_element_type=F32)
        over_tiles(body)

    def finish_o(k, half):
        rs = part_rows(half)
        out_tile = width // 2

        def out_body(t, carry):
            cols = pl.ds(pl.multiple_of(t * out_tile, out_tile), out_tile)
            y = jnp.dot(q[...], wout[:, cols], preferred_element_type=F32) + bout[:, cols]
            obuf[k, rs, cols] = (xbuf[k, rs, cols].astype(F32) + y).astype(BF16)
            return carry
        lax.fori_loop(0, width // out_tile, out_body, 0, unroll=True)

        @pl.when(k == chip)
        def _():
            pltpu.make_async_copy(obuf.at[k, rs], out_ref.at[chip, rs], or_sem.at[chip * HALVES + half]).start()

        @pl.when(k != chip)
        def _():
            out_copy(k, half).start()

    lead = jnp.int32(0)
    for c, (k, _, _) in enumerate(LEADS):
        lead = jnp.where(chip == c, k, lead)
    length = max(len(steps) for steps in SCHEDULES)
    words = []
    for first in range(0, length, PER_WORD):
        word = jnp.int32(0)
        for c, steps in enumerate(SCHEDULES):
            word = jnp.where(me == c, pack(steps[first:first + PER_WORD]), word)
        words.append(word)

    def step(i, carry):
        code = words[0]
        for n in range(1, len(words)):
            code = jnp.where(i >= n * PER_WORD, words[n], code)
        action = lax.shift_right_logical(code, BITS * (i % PER_WORD)) % (1 << BITS)

        @pl.when(action < W)
        def _():
            do_v(action // HALVES, action % HALVES)

        @pl.when(jnp.logical_and(action >= W, action < O_FIRST))
        def _():
            each_vn_copy(action - W, lambda cp: cp.wait_recv())

        @pl.when(jnp.logical_and(action >= O_FIRST, action < G))
        def _():
            do_o((action - O_FIRST) // HALVES, action % HALVES)

        @pl.when(action == G)
        def _():
            gates(far, (HALVES - 1) * part, part, False)

        @pl.when(action == PART)
        def _():
            do_part()

        @pl.when(action == LEAD)
        def _():
            do_lead()

        @pl.when(action == OWN)
        def _():
            do_own_term()

        @pl.when(action == LAST)
        def _():
            do_last()
        return carry
    do_own()
    do_mask()
    lax.fori_loop(0, length, step, 0)

    for d in range(1, chips):
        for half in range(HALVES):
            x_copy(d, half).wait_send()
    for k in range(chips):
        each_vn_copy(k, lambda cp: cp.wait_send())

        @pl.when(k != chip)
        def _():
            for half in range(HALVES):
                out_copy(k, half).wait_send()
    for k in range(chips):
        for half in range(HALVES):
            rs = part_rows(half)
            pltpu.make_async_copy(out_ref.at[k, rs], out_ref.at[k, rs], or_sem.at[k * HALVES + half]).wait()


def solution(mesh):
    row_spec = P('data', 'seq', None)
    replicated = P()

    def local_block(act_in, ln1_scale, ln1_bias, w_in, b_in, ln2_scale, ln2_bias, w_spatial, b_spatial, causal_mask, w_out, b_out):
        chips, rows, width = act_in.shape
        cores = mesh.shape['seq'] // chips
        ffn, gate, total = w_in.shape[1], w_out.shape[0], w_spatial.shape[0]
        any_spec = pl.BlockSpec(memory_space=pl.ANY)
        row = lambda a: a.reshape(1, -1)
        dma = pltpu.SemaphoreType.DMA
        return pl.pallas_call(
            functools.partial(kernel, cores),
            out_shape=pltpu.VMEM(act_in.shape, act_in.dtype),
            in_specs=[any_spec] * 12,
            out_specs=pl.BlockSpec(memory_space=pltpu.VMEM),
            scratch_shapes=[
                pltpu.VMEM((chips, rows, width), BF16),
                pltpu.VMEM((rows, width), BF16),
                pltpu.VMEM((rows, gate), BF16),
                pltpu.VMEM((chips, rows, gate), BF16),
                pltpu.VMEM((total, gate), BF16),
                pltpu.VMEM((chips, rows, total), BF16),
                pltpu.VMEM((chips, rows, total), jnp.int32),
                pltpu.VMEM((width, ffn), BF16),
                pltpu.VMEM((gate, width), BF16),
                pltpu.VMEM((rows // HALVES, gate), BF16),
                pltpu.VMEM((rows // HALVES, gate), F32),
                pltpu.VMEM((chips, rows, width), BF16),
                pltpu.VMEM((1, width), F32),
                pltpu.VMEM((1, width), F32),
                pltpu.VMEM((1, ffn), F32),
                pltpu.VMEM((1, gate), F32),
                pltpu.VMEM((1, gate), F32),
                pltpu.VMEM((1, total), F32),
                pltpu.VMEM((1, width), F32),
                dma((7,)), dma((2,)), dma, dma((chips,)), dma((chips,)),
                dma(((chips - 1) * HALVES,)), dma((chips * HALVES,)), dma((chips * PIECES,)), dma((chips * PIECES,)), dma((chips * HALVES,)), dma((chips * HALVES,)),
            ],
            compiler_params=pltpu.CompilerParams(collective_id=0, has_side_effects=True, vmem_limit_bytes=60_000_000),
        )(act_in, row(ln1_scale), row(ln1_bias), w_in, row(b_in), row(ln2_scale), row(ln2_bias), w_spatial, row(b_spatial),
          causal_mask, w_out, row(b_out))

    return jax.shard_map(local_block, mesh=mesh, in_specs=(row_spec,) + (replicated,) * 11, out_specs=row_spec, check_vma=False)
```
